8 devices in a mesh: dp: 1 (over z), sp: 8 (over y, x, core).
Axes of the slice: x: 2, y: 2, z: 1, core: 2. Of those that a mesh axis runs over, the one named last changes fastest.
Arguments:
- hidden: bfloat16 [1024, 2560], P(('dp', 'sp'))
- ln_gain: bfloat16 [2560], replicated
- w_q: bfloat16 [2560, 4096], replicated
- w_k: bfloat16 [2560, 1024], replicated
- w_v: bfloat16 [2560, 1024], replicated
- w_o: bfloat16 [4096, 2560], replicated
- q_gain: bfloat16 [128], replicated
- k_gain: bfloat16 [128], replicated
Outputs:
- output: bfloat16 [1024, 2560], P(('dp', 'sp'))
All inputs are finite; a program needn't handle non-finite values.
Results may differ from the reference program's by a relative error of at most 0.00712467.
Values are sent between devices in bfloat16 or wider.
A program may use at most 1 GiB of HBM per device.

```python
import math
import jax
import jax.numpy as jnp
from jax import lax

D = 2560
HEADS = 32
KV_HEADS = 8
HEAD = 128
SEQ = 1024
EPS = 1e-6
THETA = 1000000.0


def setup_inputs(seed: int = 0, part: int = 0) -> dict:
    keys = jax.random.split(jax.random.key(seed), 7)
    part_key = jax.random.fold_in(jax.random.key(seed + 1), part)
    gain_scale = math.log(SEQ / 8.0) ** 0.25
    hidden = jax.random.normal(part_key, (SEQ, D), jnp.float32)
    ln_gain = 1.0 + 0.3 * jax.random.normal(keys[0], (D,), jnp.float32)
    w_q = jax.random.normal(keys[1], (D, HEADS * HEAD), jnp.float32) * D ** -0.5
    w_k = jax.random.normal(keys[2], (D, KV_HEADS * HEAD), jnp.float32) * D ** -0.5
    w_v = jax.random.normal(keys[3], (D, KV_HEADS * HEAD), jnp.float32) * D ** -0.5
    w_o = jax.random.normal(keys[4], (HEADS * HEAD, D), jnp.float32) * (2.0 * (HEADS * HEAD) ** -0.5)
    q_gain = gain_scale * (1.0 + 0.2 * jax.random.normal(keys[5], (HEAD,), jnp.float32))
    k_gain = gain_scale * (1.0 + 0.2 * jax.random.normal(keys[6], (HEAD,), jnp.float32))
    return {
        'hidden': hidden.astype(jnp.bfloat16),
        'ln_gain': ln_gain.astype(jnp.bfloat16),
        'w_q': w_q.astype(jnp.bfloat16),
        'w_k': w_k.astype(jnp.bfloat16),
        'w_v': w_v.astype(jnp.bfloat16),
        'w_o': w_o.astype(jnp.bfloat16),
        'q_gain': q_gain.astype(jnp.bfloat16),
        'k_gain': k_gain.astype(jnp.bfloat16),
    }


def head_norm(values, gain):
    return values * lax.rsqrt(jnp.mean(values * values, axis=-1, keepdims=True) + EPS) * gain.astype(jnp.float32)


def rotate(values, positions):
    half = HEAD // 2
    inv_freq = jnp.power(THETA, -(jnp.arange(half, dtype=jnp.float32) * (2.0 / HEAD)))
    angles = positions.astype(jnp.float32)[:, None] * inv_freq[None, :]
    cos_pos = jnp.cos(angles)[:, None, :]
    sin_pos = jnp.sin(angles)[:, None, :]
    first_half = values[..., :half]
    second_half = values[..., half:]
    return jnp.concatenate([first_half * cos_pos - second_half * sin_pos, second_half * cos_pos + first_half * sin_pos], axis=-1)


def attend(q_all, k_all, v_all):
    limit = 2 ** 25 // (HEADS * SEQ)
    block_rows = min(SEQ, 2 ** max(3, min(9, limit.bit_length() - 1)))
    num_blocks = SEQ // block_rows
    group = HEADS // KV_HEADS
    q_blocks = q_all.reshape(num_blocks, block_rows, KV_HEADS, group, HEAD)
    key_pos = jnp.arange(SEQ)
    k_f32 = k_all.astype(jnp.float32)
    v_f32 = v_all.astype(jnp.float32)

    def one_block(block_args):
        q_block, block_idx = block_args
        scores = jnp.einsum('qkgd,skd->kgqs', q_block.astype(jnp.float32), k_f32) * (HEAD ** -0.5)
        q_pos = block_idx * block_rows + jnp.arange(block_rows)
        visible = q_pos[:, None] >= key_pos[None, :]
        scores = jnp.where(visible, scores, -jnp.inf)
        attn_prob = jax.nn.softmax(scores, axis=-1).astype(jnp.bfloat16)
        mixed = jnp.einsum('kgqs,skd->qkgd', attn_prob.astype(jnp.float32), v_f32)
        return mixed.astype(jnp.bfloat16)

    outputs = lax.map(one_block, (q_blocks, jnp.arange(num_blocks)))
    return outputs.reshape(SEQ, HEADS, HEAD)


def reference(hidden, ln_gain, w_q, w_k, w_v, w_o, q_gain, k_gain):
    hidden_f32 = hidden.astype(jnp.float32)
    normed = (hidden_f32 * lax.rsqrt(jnp.mean(hidden_f32 * hidden_f32, axis=-1, keepdims=True) + EPS) * ln_gain.astype(jnp.float32)).astype(jnp.bfloat16)
    positions = jnp.arange(SEQ)
    q_raw = jnp.dot(normed, w_q, preferred_element_type=jnp.float32).reshape(SEQ, HEADS, HEAD)
    k_raw = jnp.dot(normed, w_k, preferred_element_type=jnp.float32).reshape(SEQ, KV_HEADS, HEAD)
    v_all = jnp.dot(normed, w_v, preferred_element_type=jnp.float32).astype(jnp.bfloat16).reshape(SEQ, KV_HEADS, HEAD)
    q_all = rotate(head_norm(q_raw, q_gain), positions).astype(jnp.bfloat16)
    k_all = rotate(head_norm(k_raw, k_gain), positions).astype(jnp.bfloat16)
    mixed = attend(q_all, k_all, v_all)
    result = hidden_f32 + jnp.dot(mixed.reshape(SEQ, HEADS * HEAD), w_o, preferred_element_type=jnp.float32)
    return result.astype(jnp.bfloat16)
```

```python
import functools

import jax
import jax.numpy as jnp
import numpy as np
from jax import lax
from jax.experimental import pallas as pl
from jax.experimental.pallas import tpu as pltpu
from jax.sharding import PartitionSpec as P

EPS = 1e-6
THETA = 1000000.0
MESH = pl.DeviceIdType.MESH
F32 = jnp.float32
BF16 = jnp.bfloat16
LANES = 128
LOG2E = 1.4426950408889634


def rope_table(seq, head_dim):
    half = head_dim // 2
    inv_freq = np.power(np.float32(THETA), -(np.arange(half, dtype=np.float32) * np.float32(2.0 / head_dim))).astype(np.float32)
    angles = (np.arange(seq, dtype=np.float32)[:, None] * inv_freq[None, :]).astype(np.float32).astype(np.float64)
    return np.concatenate([np.cos(angles), np.sin(angles)], axis=1).astype(np.float32)


def kernel(x_hbm, ln_gain, w_q, w_k, w_v, w_o, q_gain, k_gain, tab_hbm, out_hbm,
           x_v, h_v, tab_v, wk_v, wv_v, wq_v, wo_v, kbuf, vbuf, qbuf, m_s, acc_s, res, out_v,
           in_sem, wk_sem, wv_sem, wq_sem, wo_sem, out_sem,
           own_sem, fwd_sem, relay_sem, krecv, vrecv):
    rows, d = x_v.shape
    n_kv, seq, hd = kbuf.shape
    group = qbuf.shape[1] // rows
    n_pairs = wk_v.shape[0]
    chips = seq // (2 * rows)
    block = 2 * rows
    me = lax.axis_index("sp")
    core = lax.rem(me, 2)
    chip = me // 2
    sibling = me + 1 - 2 * core
    score_scale = hd ** -0.5 * LOG2E

    x_copy = pltpu.make_async_copy(x_hbm, x_v, in_sem.at[0])
    tab_copy = pltpu.make_async_copy(tab_hbm.at[pl.ds(pl.multiple_of(me * rows, rows), rows)], tab_v, in_sem.at[1])
    x_copy.start()

    def wk_copy(p):
        return pltpu.make_async_copy(w_k.at[:, pl.ds(pl.multiple_of(p * 2 * hd, 2 * hd), 2 * hd)], wk_v.at[p], wk_sem.at[p])

    def wv_copy(p):
        return pltpu.make_async_copy(w_v.at[:, pl.ds(pl.multiple_of(p * 2 * hd, 2 * hd), 2 * hd)], wv_v.at[p], wv_sem.at[p])

    def wq_copy(h):
        n = group * hd
        return pltpu.make_async_copy(w_q.at[:, pl.ds(pl.multiple_of(h * n, n), n)], wq_v.at[h], wq_sem.at[h])

    def wo_copy(h):
        n = group * hd
        return pltpu.make_async_copy(w_o.at[pl.ds(pl.multiple_of(h * n, n), n)], wo_v.at[h], wo_sem.at[h])

    wk_copy(0).start()
    wv_copy(0).start()
    tab_copy.start()
    for p in range(1, n_pairs):
        wk_copy(p).start()
        wv_copy(p).start()
    for h in range(n_kv):
        wq_copy(h).start()
        wo_copy(h).start()

    barrier = pltpu.get_barrier_semaphore()
    pl.semaphore_signal(barrier, inc=1, device_id={"sp": sibling}, device_id_type=MESH)
    for step in range(1, chips):
        pl.semaphore_signal(barrier, inc=1, device_id={"sp": lax.rem(me + 2 * step, 2 * chips)}, device_id_type=MESH)

    def send(buf, h, src, dst, sem):
        part = buf.at[h, pl.ds(pl.multiple_of(src * rows, rows), rows)]
        recv = krecv if buf is kbuf else vrecv
        return pltpu.make_async_remote_copy(src_ref=part, dst_ref=part, send_sem=sem, recv_sem=recv.at[h, src],
                                            device_id={"sp": dst}, device_id_type=MESH)

    def arrived(buf, h, src):
        send(buf, h, src, sibling, fwd_sem.at[0, 0, 0]).wait_recv()

    x_copy.wait()
    xf = x_v[...].astype(F32)
    res[...] = xf
    norm = lax.rsqrt(jnp.mean(xf * xf, axis=-1, keepdims=True) + EPS)
    h_v[...] = (xf * norm * ln_gain[...].astype(F32)).astype(BF16)
    tab_copy.wait()
    table = tab_v[...]
    turned = pltpu.roll(table, hd // 2, 1)
    low = lax.broadcasted_iota(jnp.int32, table.shape, 1) < hd // 2
    cos_pos = jnp.where(low, table, turned)
    sin_pos = jnp.where(low, -turned, table)

    def head_norm_rotate(values, gain):
        gain = jnp.broadcast_to(gain[...].astype(F32), (8, hd))
        gain_turned = pltpu.roll(gain, hd // 2, 1)
        values = values * lax.rsqrt(jnp.mean(values * values, axis=-1, keepdims=True) + EPS)
        return (values * (cos_pos * gain[:1]) + pltpu.roll(values, hd // 2, 1) * (sin_pos * gain_turned[:1])).astype(BF16)

    my_rows = pl.ds(pl.multiple_of(me * rows, rows), rows)
    pl.semaphore_wait(barrier, chips)

    def send_own_far(h):
        send(vbuf, h, me, me + 2, own_sem.at[1, 1, h]).start()
        send(kbuf, h, me, me + 2, own_sem.at[0, 1, h]).start()

    def kv_pair(p, carry):
        wk_copy(p).wait()
        wv_copy(p).wait()
        keys = jnp.dot(h_v[...], wk_v[p], preferred_element_type=F32)
        vals = jnp.dot(h_v[...], wv_v[p], preferred_element_type=F32)
        for j in range(2):
            h = 2 * p + j
            cols = slice(j * hd, (j + 1) * hd)
            vbuf[h, my_rows, :] = vals[:, cols].astype(BF16)
            kbuf[h, my_rows, :] = head_norm_rotate(keys[:, cols], k_gain)
        for j in range(2):
            h = 2 * p + j
            send(kbuf, h, me, sibling, own_sem.at[0, 0, h]).start()
            send(vbuf, h, me, sibling, own_sem.at[1, 0, h]).start()

            @pl.when(chip == 0)
            def _():
                send(kbuf, h, me, me + 6, own_sem.at[0, 3, h]).start()
                send(vbuf, h, me, me + 2, own_sem.at[1, 1, h]).start()
                send(kbuf, h, me, me + 2, own_sem.at[0, 1, h]).start()
                send(vbuf, h, me, me + 4, own_sem.at[1, 2, h]).start()
                send(kbuf, h, me, me + 4, own_sem.at[0, 2, h]).start()

            @pl.when(chip == 1)
            def _():
                send(vbuf, h, me, me + 4, own_sem.at[1, 2, h]).start()
                send(kbuf, h, me, me + 4, own_sem.at[0, 2, h]).start()
                send(kbuf, h, me, me + 2, own_sem.at[0, 1, h]).start()

            @pl.when((chip == 2) & (p == 0))
            def _():
                send_own_far(h)
        return carry

    lax.fori_loop(0, n_pairs, kv_pair, 0)

    def project_q(h):
        wq_copy(h).wait()
        q = jnp.dot(h_v[...], wq_v[h], preferred_element_type=F32)
        for g in range(group):
            qbuf[h, g * rows:(g + 1) * rows, :] = head_norm_rotate(q[:, g * hd:(g + 1) * hd], q_gain)

    def relay(h):
        @pl.when(chip >= 2)
        def _():
            src = 2 * (chip - 2) + core
            arrived(vbuf, h, src)
            send(vbuf, h, src, 2 * (5 - chip) + core, relay_sem.at[h]).start()
            send(vbuf, h, src, sibling, fwd_sem.at[1, chip - 2, h]).start()

    def forward(buf, t, sc, h):
        src = 2 * sc + core
        arrived(buf, h, src)
        send(buf, h, src, sibling, fwd_sem.at[t, sc, h]).start()

    def direct(h):
        @pl.when(chip == 1)
        def _():
            forward(vbuf, 1, 0, h)
            forward(kbuf, 0, 0, h)

        @pl.when(chip == 2)
        def _():
            forward(kbuf, 0, 0, h)
            forward(vbuf, 1, 1, h)
            forward(kbuf, 0, 1, h)

        @pl.when(chip == 3)
        def _():
            forward(vbuf, 1, 2, h)
            forward(kbuf, 0, 2, h)
            forward(kbuf, 0, 1, h)
            forward(kbuf, 0, 0, h)
            forward(vbuf, 1, 0, h)

    ones = jnp.ones((block, hd), BF16)
    row_id = lax.broadcasted_iota(jnp.int32, (rows, block), 0)
    key_id = lax.broadcasted_iota(jnp.int32, (rows, block), 1)

    def scores_of(h, keys):
        return lax.dot_general(qbuf[h], kbuf[h, keys, :], (((1,), (1,)), ((), ())), preferred_element_type=F32)

    def weighted(probs, h, keys):
        return jnp.dot(probs, jnp.concatenate([vbuf[h, keys, :], ones], axis=1), preferred_element_type=F32)

    def attend_own(h):
        arrived(kbuf, h, sibling)
        arrived(vbuf, h, sibling)
        keys = pl.ds(pl.multiple_of(chip * block, block), block)
        scores = scores_of(h, keys)
        visible = key_id <= row_id + core * rows
        scores = jnp.where(jnp.concatenate([visible] * group, axis=0), scores, -jnp.inf)
        top = jnp.max(scores, axis=-1, keepdims=True)
        probs = jnp.exp2((scores - top) * score_scale).astype(BF16)
        m_s[...] = jnp.broadcast_to(top, m_s.shape)
        acc_s[...] = weighted(probs, h, keys)

    def attend_block(h, sc):
        arrived(kbuf, h, 2 * sc + 1 - core)
        arrived(vbuf, h, 2 * sc + 1 - core)
        keys = pl.ds(pl.multiple_of(sc * block, block), block)
        scores = scores_of(h, keys)
        old = m_s[...]
        top = jnp.maximum(old, jnp.max(scores, axis=-1, keepdims=True))
        top2 = jnp.concatenate([top, top], axis=1)
        probs = jnp.exp2((scores - top2) * score_scale).astype(BF16)
        decay = jnp.exp2((old - top) * score_scale)
        m_s[...] = top
        acc_s[...] = acc_s[...] * jnp.concatenate([decay, decay], axis=1) + weighted(probs, h, keys)

    def project_out(h):
        wo_copy(h).wait()
        mixed = (acc_s[:, :hd] / acc_s[:, hd:]).astype(BF16)
        mixed = jnp.concatenate([mixed[g * rows:(g + 1) * rows] for g in range(group)], axis=1)
        res[...] += jnp.dot(mixed, wo_v[h], preferred_element_type=F32)

    project_q(0)
    relay(0)
    project_q(1)
    relay(1)
    direct(0)
    attend_own(0)

    def head_step(h, carry):
        for sc in range(chips - 1):
            @pl.when(chip > sc)
            def _():
                attend_block(h, sc)

        @pl.when(h < n_kv - 2)
        def _():
            relay(h + 2)

            @pl.when(chip == 2)
            def _():
                send_own_far(h + 2)

        @pl.when(h < n_kv - 1)
        def _():
            direct(h + 1)

        project_out(h)

        @pl.when(h < n_kv - 2)
        def _():
            project_q(h + 2)

        @pl.when(h < n_kv - 1)
        def _():
            attend_own(h + 1)
        return carry

    lax.fori_loop(0, n_kv, head_step, 0)
    out_v[...] = res[...].astype(BF16)
    out_copy = pltpu.make_async_copy(out_v, out_hbm, out_sem)
    out_copy.start()

    def finish_sends(h, carry):
        def done(buf, src, sem):
            send(buf, h, src, sibling, sem).wait_send()

        done(kbuf, me, own_sem.at[0, 0, h])
        done(vbuf, me, own_sem.at[1, 0, h])

        @pl.when(chip <= 2)
        def _():
            done(kbuf, me, own_sem.at[0, 1, h])

        @pl.when((chip == 0) | (chip == 2))
        def _():
            done(vbuf, me, own_sem.at[1, 1, h])

        @pl.when(chip <= 1)
        def _():
            done(kbuf, me, own_sem.at[0, 2, h])
            done(vbuf, me, own_sem.at[1, 2, h])

        @pl.when(chip == 0)
        def _():
            done(kbuf, me, own_sem.at[0, 3, h])

        @pl.when(chip >= 2)
        def _():
            done(vbuf, 2 * (chip - 2) + core, relay_sem.at[h])
        for sc in range(chips - 1):
            @pl.when(chip > sc)
            def _():
                done(kbuf, 2 * sc + core, fwd_sem.at[0, sc, h])
                done(vbuf, 2 * sc + core, fwd_sem.at[1, sc, h])
        return carry

    lax.fori_loop(0, n_kv, finish_sends, 0)
    out_copy.wait()


def solution(mesh):
    def device_step(hidden, ln_gain, w_q, w_k, w_v, w_o, q_gain, k_gain):
        rows, d = hidden.shape
        hd = q_gain.shape[0]
        n_kv = w_k.shape[1] // hd
        group = w_q.shape[1] // w_k.shape[1]
        seq = rows * mesh.shape['sp']
        table = jnp.asarray(rope_table(seq, hd))
        any_spec = pl.BlockSpec(memory_space=pl.ANY)
        vmem_spec = pl.BlockSpec(memory_space=pltpu.VMEM)
        dma = pltpu.SemaphoreType.DMA
        return pl.pallas_call(
            kernel,
            out_shape=jax.ShapeDtypeStruct((rows, d), BF16),
            in_specs=[any_spec, vmem_spec, any_spec, any_spec, any_spec, any_spec, vmem_spec, vmem_spec, any_spec],
            out_specs=any_spec,
            scratch_shapes=[
                pltpu.VMEM((rows, d), BF16),
                pltpu.VMEM((rows, d), BF16),
                pltpu.VMEM((rows, hd), F32),
                pltpu.VMEM((n_kv // 2, d, 2 * hd), BF16),
                pltpu.VMEM((n_kv // 2, d, 2 * hd), BF16),
                pltpu.VMEM((n_kv, d, group * hd), BF16),
                pltpu.VMEM((n_kv, group * hd, d), BF16),
                pltpu.VMEM((n_kv, seq, hd), BF16),
                pltpu.VMEM((n_kv, seq, hd), BF16),
                pltpu.VMEM((n_kv, group * rows, hd), BF16),
                pltpu.VMEM((group * rows, LANES), F32),
                pltpu.VMEM((group * rows, 2 * hd), F32),
                pltpu.VMEM((rows, d), F32),
                pltpu.VMEM((rows, d), BF16),
                dma((2,)),
                dma((n_kv // 2,)),
                dma((n_kv // 2,)),
                dma((n_kv,)),
                dma((n_kv,)),
                dma,
                dma((2, 4, n_kv)),
                dma((2, 3, n_kv)),
                dma((n_kv,)),
                dma((n_kv, 8)),
                dma((n_kv, 8)),
            ],
            compiler_params=pltpu.CompilerParams(collective_id=0, has_side_effects=True, vmem_limit_bytes=67043328),
        )(hidden, ln_gain.reshape(1, -1), w_q, w_k, w_v, w_o, q_gain.reshape(1, -1), k_gain.reshape(1, -1), table)

    row_spec = P(('dp', 'sp'), None)
    return jax.shard_map(device_step, mesh=mesh, in_specs=(row_spec, P(), P(), P(), P(), P(), P(), P()), out_specs=row_spec, check_vma=False)
```

```python
import functools

import jax
import jax.numpy as jnp
import numpy as np
from jax import lax
from jax.experimental import pallas as pl
from jax.experimental.pallas import tpu as pltpu
from jax.sharding import PartitionSpec as P

EPS = 1e-6
THETA = 1000000.0
MESH = pl.DeviceIdType.MESH
F32 = jnp.float32
BF16 = jnp.bfloat16
LANES = 128
LOG2E = 1.4426950408889634
AHEAD = 2


def rope_table(seq, head_dim):
    half = head_dim // 2
    inv_freq = np.power(np.float32(THETA), -(np.arange(half, dtype=np.float32) * np.float32(2.0 / head_dim))).astype(np.float32)
    angles = (np.arange(seq, dtype=np.float32)[:, None] * inv_freq[None, :]).astype(np.float32).astype(np.float64)
    return np.concatenate([np.cos(angles), np.sin(angles)], axis=1).astype(np.float32)


def kernel(x_hbm, ln_gain_hbm, w_q, w_k, w_v, w_o, q_gain_hbm, k_gain_hbm, tab_hbm, out_v,
           x_v, h_v, ln_gain, q_gain, k_gain, tab_v, wk_v, wv_v, wq_v, wo_v, kbuf, vbuf, qraw, qbuf, mixed_t, res,
           in_sem, wk_sem, wv_sem, wq_sem, wo_sem,
           swap_send, swap_recv, far_sem, far_recv, fwd_send, relay_sem):
    rows, d = x_v.shape
    n_kv, n_dev, _, hd = kbuf.shape
    group = qbuf.shape[1] // rows
    n_pairs = wk_v.shape[0]
    wq_slots, wo_slots = wq_v.shape[0], wo_v.shape[0]
    chips = n_dev // 2
    me = lax.axis_index("sp")
    core = lax.rem(me, 2)
    chip = me // 2
    sibling = me + 1 - 2 * core
    score_scale = hd ** -0.5 * LOG2E

    x_copy = pltpu.make_async_copy(x_hbm, x_v, in_sem.at[0])
    small_copies = [
        pltpu.make_async_copy(ln_gain_hbm, ln_gain, in_sem.at[1]),
        pltpu.make_async_copy(q_gain_hbm, q_gain, in_sem.at[2]),
        pltpu.make_async_copy(k_gain_hbm, k_gain, in_sem.at[3]),
        pltpu.make_async_copy(tab_hbm.at[pl.ds(pl.multiple_of(me * rows, rows), rows)], tab_v, in_sem.at[4]),
    ]

    def wk_copy(p):
        return pltpu.make_async_copy(w_k.at[:, pl.ds(pl.multiple_of(p * 2 * hd, 2 * hd), 2 * hd)], wk_v.at[p], wk_sem.at[lax.rem(p, 2)])

    def wv_copy(p):
        return pltpu.make_async_copy(w_v.at[:, pl.ds(pl.multiple_of(p * 2 * hd, 2 * hd), 2 * hd)], wv_v.at[p], wv_sem.at[lax.rem(p, 2)])

    def wq_copy(h):
        n = group * hd
        slot = lax.rem(h, wq_slots)
        return pltpu.make_async_copy(w_q.at[:, pl.ds(pl.multiple_of(h * n, n), n)], wq_v.at[slot], wq_sem.at[slot])

    def wo_copy(h):
        n = group * hd
        slot = lax.rem(h, wo_slots)
        return pltpu.make_async_copy(w_o.at[pl.ds(pl.multiple_of(h * n, n), n)], wo_v.at[slot], wo_sem.at[slot])

    x_copy.start()
    for copy in small_copies:
        copy.start()
    wk_copy(0).start()
    wv_copy(0).start()

    barrier = pltpu.get_barrier_semaphore()
    for step in range(1, n_dev):
        pl.semaphore_signal(barrier, inc=1, device_id={"sp": lax.rem(me + step, n_dev)}, device_id_type=MESH)

    def swap(buf, t, h):
        part = buf.at[h, me]
        return pltpu.make_async_remote_copy(src_ref=part, dst_ref=part, send_sem=swap_send.at[t], recv_sem=swap_recv.at[t, h],
                                            device_id={"sp": sibling}, device_id_type=MESH)

    def swapped(buf, t, h):
        part = buf.at[h, sibling]
        pltpu.make_async_remote_copy(src_ref=part, dst_ref=part, send_sem=swap_send.at[t], recv_sem=swap_recv.at[t, h],
                                     device_id={"sp": sibling}, device_id_type=MESH).wait_recv()

    def send(buf, h, sc, dst, sem):
        part = buf.at[h, pl.ds(2 * sc, 2)]
        t = 0 if buf is kbuf else 1
        return pltpu.make_async_remote_copy(src_ref=part, dst_ref=part, send_sem=sem, recv_sem=far_recv.at[t, h, sc],
                                            device_id={"sp": dst}, device_id_type=MESH)

    def arrived(buf, h, sc):
        send(buf, h, sc, sibling, fwd_send.at[0]).wait_recv()

    with jax.named_scope("gain_wait"):
        small_copies[0].wait()
    gain_rows = ln_gain[...].astype(F32)

    with jax.named_scope("x_wait"):
        x_copy.wait()
    wk_copy(1).start()
    wv_copy(1).start()
    for r in range(0, rows, 16):
        xf = x_v[r:r + 16, :].astype(F32)
        norm = lax.rsqrt(jnp.mean(xf * xf, axis=-1, keepdims=True) + EPS)
        for c in range(d // LANES):
            cols = slice(c * LANES, (c + 1) * LANES)
            h_v[r:r + 16, cols] = (xf[:, cols] * norm * gain_rows[c:c + 1, :]).astype(BF16)

    with jax.named_scope("small_wait"):
        for copy in small_copies[1:]:
            copy.wait()
    table = tab_v[...]
    turned = pltpu.roll(table, hd // 2, 1)
    low = lax.broadcasted_iota(jnp.int32, table.shape, 1) < hd // 2
    cos_pos = jnp.where(low, table, turned)
    sin_pos = jnp.where(low, -turned, table)

    def head_norm_rotate(values, gain):
        gain = jnp.broadcast_to(gain[...].astype(F32), (8, hd))
        gain_turned = pltpu.roll(gain, hd // 2, 1)
        values = values * lax.rsqrt(jnp.mean(values * values, axis=-1, keepdims=True) + EPS)
        return (values * (cos_pos * gain[:1]) + pltpu.roll(values, hd // 2, 1) * (sin_pos * gain_turned[:1])).astype(BF16)

    with jax.named_scope("barrier"):
        pl.semaphore_wait(barrier, n_dev - 1)

    def far_send(h):
        @pl.when((chip == 0) & (core == 1))
        def _():
            send(vbuf, h, 0, 3, far_sem.at[0]).start()
            send(kbuf, h, 0, 6, far_sem.at[1]).start()
            send(kbuf, h, 0, 2, far_sem.at[2]).start()

        @pl.when((chip == 0) & (core == 0))
        def _():
            send(vbuf, h, 0, 5, far_sem.at[0]).start()
            send(kbuf, h, 0, 4, far_sem.at[1]).start()

        @pl.when((chip == 1) & (core == 0))
        def _():
            send(vbuf, h, 1, 7, far_sem.at[0]).start()
            send(kbuf, h, 1, 6, far_sem.at[1]).start()

        @pl.when((chip == 1) & (core == 1))
        def _():
            send(kbuf, h, 1, 4, far_sem.at[1]).start()

        @pl.when((chip == 2) & (core == 1))
        def _():
            send(vbuf, h, 2, 7, far_sem.at[0]).start()
            send(kbuf, h, 2, 6, far_sem.at[1]).start()

    def swap_in(p):
        with jax.named_scope("swap_in"):
            for j in range(2):
                swapped(kbuf, 0, 2 * p + j)
                swapped(vbuf, 1, 2 * p + j)

        @pl.when(p < AHEAD // 2)
        def _():
            far_send(2 * p)
            far_send(2 * p + 1)

    def kv_pair(p, carry):
        with jax.named_scope("wkv_wait"):
            wk_copy(p).wait()
            wv_copy(p).wait()

        @pl.when(p < n_pairs - 2)
        def _():
            wk_copy(p + 2).start()
            wv_copy(p + 2).start()

        @pl.when(p >= n_pairs - 2)
        def _():
            wq_copy(p - (n_pairs - 2)).start()

        keys = jnp.dot(h_v[...], wk_v[p], preferred_element_type=F32)
        vals = jnp.dot(h_v[...], wv_v[p], preferred_element_type=F32)
        for j in range(2):
            h = 2 * p + j
            cols = slice(j * hd, (j + 1) * hd)
            kbuf[h, me] = head_norm_rotate(keys[:, cols], k_gain)
            vbuf[h, me] = vals[:, cols].T.astype(BF16)
        for j in range(2):
            swap(kbuf, 0, 2 * p + j).start()
            swap(vbuf, 1, 2 * p + j).start()

        @pl.when(p > 0)
        def _():
            swap_in(p - 1)
        return carry

    lax.fori_loop(0, n_pairs, kv_pair, 0)

    def q_dot(h):
        qraw[lax.rem(h, 2)] = jnp.dot(h_v[...], wq_v[lax.rem(h, wq_slots)], preferred_element_type=F32)

    def q_finish(h):
        q = qraw[lax.rem(h, 2)]
        for g in range(group):
            qbuf[h, g * rows:(g + 1) * rows, :] = head_norm_rotate(q[:, g * hd:(g + 1) * hd], q_gain)

    def wq_wait(h):
        with jax.named_scope("wq_wait"):
            wq_copy(h).wait()

    @jax.named_scope("relay")
    def relay(h):
        @pl.when((chip >= 2) & (core == 1))
        def _():
            sc = chip - 2
            arrived(vbuf, h, sc)
            send(vbuf, h, sc, 11 - 2 * chip, relay_sem).start()
            send(vbuf, h, sc, sibling, fwd_send.at[sc]).start()

    def forward(buf, h, sc):
        arrived(buf, h, sc)
        send(buf, h, sc, sibling, fwd_send.at[sc]).start()

    @jax.named_scope("direct")
    def direct(h):
        @pl.when((chip >= 1) & (core == 0))
        def _():
            for sc in range(chips - 2, -1, -1):
                @pl.when(chip > sc)
                def _():
                    forward(kbuf, h, sc)

        @pl.when((chip >= 1) & (core == 1))
        def _():
            for sc in range(chips - 2, -1, -1):
                @pl.when((chip > sc) & (chip != sc + 2))
                def _():
                    forward(vbuf, h, sc)

    def attend(h, c):
        if c:
            with jax.named_scope("block_wait"):
                for sc in range(c - 1, -1, -1):
                    @pl.when(core == 0)
                    def _():
                        arrived(vbuf, h, sc)

                    @pl.when(core == 1)
                    def _():
                        arrived(kbuf, h, sc)
        n_keys = 2 * (c + 1) * rows
        keys = kbuf[h, 0:2 * (c + 1)].reshape(n_keys, hd)
        scores = lax.dot_general(keys, qbuf[h], (((1,), (1,)), ((), ())), preferred_element_type=F32)
        key_id = lax.broadcasted_iota(jnp.int32, (2 * rows, rows), 0)
        row_id = lax.broadcasted_iota(jnp.int32, (2 * rows, rows), 1)
        visible = jnp.concatenate([key_id <= row_id + core * rows] * group, axis=1)
        last = jnp.where(visible, scores[n_keys - 2 * rows:], -jnp.inf)
        scores = jnp.concatenate([scores[:n_keys - 2 * rows], last], axis=0) if c else last
        top = jnp.max(scores, axis=0, keepdims=True)
        probs = jnp.exp2((scores - top) * score_scale)
        total = jnp.sum(probs, axis=0, keepdims=True)
        vals = jnp.concatenate([vbuf[h, src] for src in range(2 * (c + 1))], axis=1)
        mixed = jnp.dot(vals, probs.astype(BF16), preferred_element_type=F32)
        mixed_t[...] = (mixed / total).astype(BF16)

    def out_dot():
        mixed = jnp.concatenate([mixed_t[:, g * rows:(g + 1) * rows].T for g in range(group)], axis=1)
        return mixed

    def project_out(h, mixed):
        res[...] += jnp.dot(mixed, wo_v[lax.rem(h, wo_slots)], preferred_element_type=F32)

    wq_copy(2).start()
    wo_copy(0).start()
    swap_in(n_pairs - 1)
    wq_wait(0)
    q_dot(0)
    relay(0)
    wq_copy(3).start()
    wo_copy(1).start()
    wq_wait(1)
    with jax.named_scope("q_first"):
        q_finish(0)
        q_dot(1)
    relay(1)
    direct(0)
    for r in range(0, rows, 16):
        res[r:r + 16, :] = x_v[r:r + 16, :].astype(F32)

    def head_step(h, carry):
        for c in range(chips):
            @pl.when(chip == c)
            @jax.named_scope("attend")
            def _():
                attend(h, c)

        @pl.when(h < n_kv - 2)
        def _():
            relay(h + 2)

        @pl.when(h < n_kv - AHEAD)
        def _():
            far_send(h + AHEAD)

        @pl.when(h < n_kv - 1)
        def _():
            direct(h + 1)

        with jax.named_scope("wo_wait"):
            wo_copy(h).wait()

        @pl.when(h < n_kv - 2)
        def _():
            wo_copy(h + 2).start()
            wq_wait(h + 2)

        @pl.when(h < n_kv - 4)
        def _():
            wq_copy(h + 4).start()

        @pl.when(h < n_kv - 2)
        @jax.named_scope("project")
        def _():
            q_finish(h + 1)
            mixed = out_dot()
            project_out(h, mixed)
            q_dot(h + 2)

        @pl.when(h >= n_kv - 2)
        @jax.named_scope("project_end")
        def _():
            @pl.when(h == n_kv - 2)
            def _():
                q_finish(h + 1)
            project_out(h, out_dot())
        return carry

    lax.fori_loop(0, n_kv, head_step, 0)
    out_v[...] = res[...].astype(BF16)

    def finish(buf, sc, sem):
        part = buf.at[:, pl.ds(2 * sc, 2)]
        pltpu.make_async_remote_copy(src_ref=part, dst_ref=part, send_sem=sem, recv_sem=far_recv.at[0, 0, 0],
                                     device_id={"sp": sibling}, device_id_type=MESH).wait_send()

    with jax.named_scope("finish_sends"):
        for t, buf in enumerate((kbuf, vbuf)):
            part = buf.at[:, me]
            pltpu.make_async_remote_copy(src_ref=part, dst_ref=part, send_sem=swap_send.at[t], recv_sem=far_recv.at[0, 0, 0],
                                         device_id={"sp": sibling}, device_id_type=MESH).wait_send()

        @pl.when((chip == 0) | ((chip + core == 1) | (chip + core == 3)) & (chip < 3))
        def _():
            finish(vbuf, 0, far_sem.at[0])

        @pl.when((chip < 2) | ((chip == 2) & (core == 1)))
        def _():
            finish(kbuf, 0, far_sem.at[1])

        @pl.when((chip == 0) & (core == 1))
        def _():
            finish(kbuf, 0, far_sem.at[2])

        @pl.when((chip >= 2) & (core == 1))
        def _():
            finish(vbuf, 0, relay_sem)
        for sc in range(chips - 1):
            @pl.when(chip > sc)
            def _():
                finish(kbuf, sc, fwd_send.at[sc])


def write_back(res_v, out_hbm, sem):
    copy = pltpu.make_async_copy(res_v, out_hbm, sem)
    copy.start()
    copy.wait()


def solution(mesh):
    def device_step(hidden, ln_gain, w_q, w_k, w_v, w_o, q_gain, k_gain):
        rows, d = hidden.shape
        hd = q_gain.shape[0]
        n_kv = w_k.shape[1] // hd
        group = w_q.shape[1] // w_k.shape[1]
        n_dev = mesh.shape['sp']
        table = jnp.asarray(rope_table(rows * n_dev, hd))
        any_spec = pl.BlockSpec(memory_space=pl.ANY)
        vmem_spec = pl.BlockSpec(memory_space=pltpu.VMEM)
        dma = pltpu.SemaphoreType.DMA
        result = pl.pallas_call(
            kernel,
            out_shape=pltpu.VMEM((rows, d), BF16),
            in_specs=[any_spec] * 9,
            out_specs=vmem_spec,
            scratch_shapes=[
                pltpu.VMEM((rows, d), BF16),
                pltpu.VMEM((rows, d), BF16),
                pltpu.VMEM((d // LANES, LANES), BF16),
                pltpu.VMEM((1, hd), BF16),
                pltpu.VMEM((1, hd), BF16),
                pltpu.VMEM((rows, hd), F32),
                pltpu.VMEM((n_kv // 2, d, 2 * hd), BF16),
                pltpu.VMEM((n_kv // 2, d, 2 * hd), BF16),
                pltpu.VMEM((5, d, group * hd), BF16),
                pltpu.VMEM((4, group * hd, d), BF16),
                pltpu.VMEM((n_kv, n_dev, rows, hd), BF16),
                pltpu.VMEM((n_kv, n_dev, hd, rows), BF16),
                pltpu.VMEM((2, rows, group * hd), F32),
                pltpu.VMEM((n_kv, group * rows, hd), BF16),
                pltpu.VMEM((hd, group * rows), BF16),
                pltpu.VMEM((rows, d), F32),
                dma((5,)),
                dma((2,)),
                dma((2,)),
                dma((5,)),
                dma((4,)),
                dma((2,)),
                dma((2, n_kv)),
                dma((3,)),
                dma((2, n_kv, n_dev // 2 - 1)),
                dma((n_dev // 2 - 1,)),
                dma,
            ],
            compiler_params=pltpu.CompilerParams(collective_id=0, has_side_effects=True, vmem_limit_bytes=62000000),
        )(hidden, ln_gain.reshape(-1, LANES), w_q, w_k, w_v, w_o, q_gain.reshape(1, -1), k_gain.reshape(1, -1), table)
        return pl.pallas_call(
            write_back,
            out_shape=jax.ShapeDtypeStruct((rows, d), BF16),
            in_specs=[vmem_spec],
            out_specs=any_spec,
            scratch_shapes=[dma],
            compiler_params=pltpu.CompilerParams(vmem_limit_bytes=1000000),
        )(result)

    row_spec = P(('dp', 'sp'), None)
    return jax.shard_map(device_step, mesh=mesh, in_specs=(row_spec, P(), P(), P(), P(), P(), P(), P()), out_specs=row_spec, check_vma=False)
```

```python
import functools

import jax
import jax.numpy as jnp
import numpy as np
from jax import lax
from jax.experimental import pallas as pl
from jax.experimental.pallas import tpu as pltpu
from jax.sharding import PartitionSpec as P

EPS = 1e-6
THETA = 1000000.0
MESH = pl.DeviceIdType.MESH
F32 = jnp.float32
BF16 = jnp.bfloat16
LANES = 128
LOG2E = 1.4426950408889634
AHEAD = 2
PARTS = 1


def rope_table(seq, head_dim):
    half = head_dim // 2
    inv_freq = np.power(np.float32(THETA), -(np.arange(half, dtype=np.float32) * np.float32(2.0 / head_dim))).astype(np.float32)
    angles = (np.arange(seq, dtype=np.float32)[:, None] * inv_freq[None, :]).astype(np.float32).astype(np.float64)
    return np.concatenate([np.cos(angles), np.sin(angles)], axis=1).astype(np.float32)


def kernel(x_hbm, ln_gain_hbm, w_q, w_k, w_v, w_o, q_gain_hbm, k_gain_hbm, tab_hbm, out_v,
           x_v, h_v, ln_gain, q_gain, k_gain, tab_v, wk_v, wv_v, wq_v, wo_v, kbuf, vbuf, qraw, qbuf, mixed_t, res,
           in_sem, wk_sem, wv_sem, wq_sem, wo_sem,
           swap_send, swap_recv, far_sem, far_recv, fwd_send, relay_sem):
    rows, d = x_v.shape
    n_kv, n_dev, _, hd = kbuf.shape
    group = qbuf.shape[1] // rows
    n_pairs = wk_v.shape[0]
    wq_slots, wo_slots = wq_v.shape[0], wo_v.shape[0]
    chips = n_dev // 2
    me = lax.axis_index("sp")
    core = lax.rem(me, 2)
    chip = me // 2
    sibling = me + 1 - 2 * core
    score_scale = hd ** -0.5 * LOG2E

    x_copy = pltpu.make_async_copy(x_hbm, x_v, in_sem.at[0])
    small_copies = [
        pltpu.make_async_copy(ln_gain_hbm, ln_gain, in_sem.at[1]),
        pltpu.make_async_copy(q_gain_hbm, q_gain, in_sem.at[2]),
        pltpu.make_async_copy(k_gain_hbm, k_gain, in_sem.at[3]),
        pltpu.make_async_copy(tab_hbm.at[pl.ds(pl.multiple_of(me * rows, rows), rows)], tab_v, in_sem.at[4]),
    ]

    def wk_copy(p):
        return pltpu.make_async_copy(w_k.at[:, pl.ds(pl.multiple_of(p * 2 * hd, 2 * hd), 2 * hd)], wk_v.at[p], wk_sem.at[lax.rem(p, 2)])

    def wv_copy(p):
        return pltpu.make_async_copy(w_v.at[:, pl.ds(pl.multiple_of(p * 2 * hd, 2 * hd), 2 * hd)], wv_v.at[p], wv_sem.at[lax.rem(p, 2)])

    def wq_copy(h):
        n = group * hd
        slot = lax.rem(h, wq_slots)
        return pltpu.make_async_copy(w_q.at[:, pl.ds(pl.multiple_of(h * n, n), n)], wq_v.at[slot], wq_sem.at[slot])

    def wo_copy(h):
        n = group * hd
        slot = lax.rem(h, wo_slots)
        return pltpu.make_async_copy(w_o.at[pl.ds(pl.multiple_of(h * n, n), n)], wo_v.at[slot], wo_sem.at[slot])

    x_copy.start()
    for copy in small_copies:
        copy.start()
    wk_copy(0).start()
    wv_copy(0).start()

    barrier = pltpu.get_barrier_semaphore()
    for step in range(1, n_dev):
        pl.semaphore_signal(barrier, inc=1, device_id={"sp": lax.rem(me + step, n_dev)}, device_id_type=MESH)

    def swap(buf, t, h):
        part = buf.at[h, me]
        return pltpu.make_async_remote_copy(src_ref=part, dst_ref=part, send_sem=swap_send.at[t], recv_sem=swap_recv.at[t, h],
                                            device_id={"sp": sibling}, device_id_type=MESH)

    def swapped(buf, t, h):
        part = buf.at[h, sibling]
        pltpu.make_async_remote_copy(src_ref=part, dst_ref=part, send_sem=swap_send.at[t], recv_sem=swap_recv.at[t, h],
                                     device_id={"sp": sibling}, device_id_type=MESH).wait_recv()

    def send(buf, h, sc, dst, sem):
        part = buf.at[h, pl.ds(2 * sc, 2)]
        t = 0 if buf is kbuf else 1
        return pltpu.make_async_remote_copy(src_ref=part, dst_ref=part, send_sem=sem, recv_sem=far_recv.at[t, h, sc],
                                            device_id={"sp": dst}, device_id_type=MESH)

    def arrived(buf, h, sc):
        send(buf, h, sc, sibling, fwd_send.at[0]).wait_recv()

    with jax.named_scope("gain_wait"):
        small_copies[0].wait()
    gain_rows = ln_gain[...].astype(F32)

    with jax.named_scope("x_wait"):
        x_copy.wait()
    wk_copy(1).start()
    wv_copy(1).start()
    for r in range(0, rows, 16):
        xf = x_v[r:r + 16, :].astype(F32)
        norm = lax.rsqrt(jnp.mean(xf * xf, axis=-1, keepdims=True) + EPS)
        for c in range(d // LANES):
            cols = slice(c * LANES, (c + 1) * LANES)
            h_v[r:r + 16, cols] = (xf[:, cols] * norm * gain_rows[c:c + 1, :]).astype(BF16)

    with jax.named_scope("small_wait"):
        for copy in small_copies[1:]:
            copy.wait()
    table = tab_v[...]
    turned = pltpu.roll(table, hd // 2, 1)
    low = lax.broadcasted_iota(jnp.int32, table.shape, 1) < hd // 2
    cos_pos = jnp.where(low, table, turned)
    sin_pos = jnp.where(low, -turned, table)

    def head_norm_rotate(values, gain):
        gain = jnp.broadcast_to(gain[...].astype(F32), (8, hd))
        gain_turned = pltpu.roll(gain, hd // 2, 1)
        values = values * lax.rsqrt(jnp.mean(values * values, axis=-1, keepdims=True) + EPS)
        return (values * (cos_pos * gain[:1]) + pltpu.roll(values, hd // 2, 1) * (sin_pos * gain_turned[:1])).astype(BF16)

    with jax.named_scope("barrier"):
        pl.semaphore_wait(barrier, n_dev - 1)

    def on(c, k):
        return pl.when((chip == c) & (core == k))

    def far_send_wide(h):
        @on(0, 1)
        def _():
            send(vbuf, h, 0, 3, far_sem.at[0]).start()
            send(kbuf, h, 0, 6, far_sem.at[1]).start()
            send(kbuf, h, 0, 2, far_sem.at[2]).start()

        @on(0, 0)
        def _():
            send(vbuf, h, 0, 5, far_sem.at[0]).start()
            send(kbuf, h, 0, 4, far_sem.at[1]).start()

        @on(1, 0)
        def _():
            send(vbuf, h, 1, 7, far_sem.at[0]).start()
            send(kbuf, h, 1, 6, far_sem.at[1]).start()

    def far_send_near(h):
        @on(2, 1)
        def _():
            send(vbuf, h, 2, 7, far_sem.at[0]).start()
            send(kbuf, h, 2, 6, far_sem.at[1]).start()

    def far_send_transit(h):
        @on(1, 1)
        def _():
            send(kbuf, h, 1, 4, far_sem.at[1]).start()

    def swap_in(p):
        with jax.named_scope("swap_in"):
            for j in range(2):
                swapped(kbuf, 0, 2 * p + j)
                swapped(vbuf, 1, 2 * p + j)

        far_send_wide(2 * p)
        far_send_wide(2 * p + 1)

        @pl.when(p == 0)
        def _():
            for h in range(AHEAD):
                far_send_near(h)

    def kv_pair(p, carry):
        with jax.named_scope("wkv_wait"):
            wk_copy(p).wait()
            wv_copy(p).wait()

        @pl.when(p < n_pairs - 2)
        def _():
            wk_copy(p + 2).start()
            wv_copy(p + 2).start()

        @pl.when(p >= n_pairs - 2)
        def _():
            wq_copy(p - (n_pairs - 2)).start()

        keys = jnp.dot(h_v[...], wk_v[p], preferred_element_type=F32)
        vals = jnp.dot(h_v[...], wv_v[p], preferred_element_type=F32)
        for j in range(2):
            h = 2 * p + j
            cols = slice(j * hd, (j + 1) * hd)
            kbuf[h, me] = head_norm_rotate(keys[:, cols], k_gain)
            vbuf[h, me] = vals[:, cols].T.astype(BF16)
        for j in range(2):
            swap(kbuf, 0, 2 * p + j).start()
            swap(vbuf, 1, 2 * p + j).start()

        @pl.when(p > 0)
        def _():
            swap_in(p - 1)
        return carry

    lax.fori_loop(0, n_pairs, kv_pair, 0)

    def q_dot(h):
        qraw[lax.rem(h, 2)] = jnp.dot(h_v[...], wq_v[lax.rem(h, wq_slots)], preferred_element_type=F32)

    def q_finish(h, slot):
        q = qraw[slot]
        for g in range(group):
            qbuf[h, g * rows:(g + 1) * rows, :] = head_norm_rotate(q[:, g * hd:(g + 1) * hd], q_gain)

    def wq_wait(h):
        with jax.named_scope("wq_wait"):
            wq_copy(h).wait()

    @jax.named_scope("relay")
    def relay(h):
        @pl.when((chip >= 2) & (core == 1))
        def _():
            sc = chip - 2
            arrived(vbuf, h, sc)
            send(vbuf, h, sc, 11 - 2 * chip, relay_sem).start()
            send(vbuf, h, sc, sibling, fwd_send.at[sc]).start()

    def forward(buf, h, sc):
        arrived(buf, h, sc)
        send(buf, h, sc, sibling, fwd_send.at[sc]).start()

    @jax.named_scope("direct")
    def direct(h):
        @pl.when((chip >= 1) & (core == 0))
        def _():
            for sc in range(chips - 2, -1, -1):
                @pl.when(chip > sc)
                def _():
                    forward(kbuf, h, sc)

        @pl.when((chip >= 1) & (core == 1))
        def _():
            for sc in range(chips - 2, -1, -1):
                @pl.when((chip > sc) & (chip != sc + 2))
                def _():
                    forward(vbuf, h, sc)

    def attend(h, c):
        if c:
            with jax.named_scope("block_wait"):
                for sc in range(c - 1, -1, -1):
                    @pl.when(core == 0)
                    def _():
                        arrived(vbuf, h, sc)

                    @pl.when(core == 1)
                    def _():
                        arrived(kbuf, h, sc)
        project_out(lax.rem(jnp.maximum(h - 1, 0), wo_slots))
        n_keys = 2 * (c + 1) * rows
        keys = kbuf[h, 0:2 * (c + 1)].reshape(n_keys, hd)
        vals = jnp.concatenate([vbuf[h, src] for src in range(2 * (c + 1))], axis=1)
        key_id = lax.broadcasted_iota(jnp.int32, (2 * rows, rows), 0)
        row_id = lax.broadcasted_iota(jnp.int32, (2 * rows, rows), 1)
        visible = key_id <= row_id + core * rows
        part = group * rows // PARTS
        visible = jnp.concatenate([visible] * (group // PARTS), axis=1)
        for i in range(PARTS):
            cols = slice(i * part, (i + 1) * part)
            scores = lax.dot_general(keys, qbuf[h, cols], (((1,), (1,)), ((), ())), preferred_element_type=F32)
            last = jnp.where(visible, scores[n_keys - 2 * rows:], -jnp.inf)
            scores = jnp.concatenate([scores[:n_keys - 2 * rows], last], axis=0) if c else last
            top = jnp.max(scores, axis=0, keepdims=True)
            probs = jnp.exp2((scores - top) * score_scale)
            total = jnp.sum(probs, axis=0, keepdims=True)
            mixed = jnp.dot(vals, probs.astype(BF16), preferred_element_type=F32)
            mixed_t[:, cols] = (mixed / total).astype(BF16)

    def project_out(slot):
        mixed = jnp.concatenate([mixed_t[:, g * rows:(g + 1) * rows].T for g in range(group)], axis=1)
        res[...] += jnp.dot(mixed, wo_v[slot], preferred_element_type=F32)

    def relay_step(h):
        relay(h)

        @pl.when(h + AHEAD < n_kv)
        def _():
            far_send_near(h + AHEAD)
        far_send_transit(h)

    wq_copy(2).start()
    wq_copy(3).start()

    def q_step(h, carry):
        wq_wait(h)

        @pl.when(h < n_kv - 4)
        def _():
            wq_copy(h + 4).start()

        @pl.when(h >= n_kv - 4)
        def _():
            wo_copy(h - (n_kv - 4)).start()

        with jax.named_scope("q_step"):
            q_finish(jnp.maximum(h - 1, 0), lax.rem(h + 1, 2))
            q_dot(h)
            some = pl.ds(pl.multiple_of(h * 16, 16), 16)
            res[some, :] = x_v[some, :].astype(F32)

        @pl.when(h == 0)
        def _():
            swap_in(n_pairs - 1)
            relay_step(0)

        @pl.when(lax.rem(h, 3) == 1)
        def _():
            relay_step(h // 3 + 1)

        @pl.when(h == n_kv - 2)
        def _():
            direct(0)
        return carry

    lax.fori_loop(0, n_kv, q_step, 0)
    with jax.named_scope("wo_wait"):
        wo_copy(0).wait()
    with jax.named_scope("q_last"):
        q_finish(n_kv - 1, (n_kv - 1) % 2)
    mixed_t[...] = jnp.zeros_like(mixed_t)

    def head_step(h, carry):
        @pl.when(h < n_kv - 1)
        def _():
            direct(h + 1)

        @pl.when(h > 1)
        @jax.named_scope("wo_wait")
        def _():
            wo_copy(h - 1).wait()

        for c in range(chips):
            @pl.when(chip == c)
            @jax.named_scope("attend")
            def _():
                attend(h, c)

        @pl.when((h > 0) & (h < n_kv - 3))
        def _():
            wo_copy(h + 3).start()

        @pl.when(h < n_kv - 4)
        def _():
            relay_step(h + 4)
        return carry

    lax.fori_loop(0, n_kv, head_step, 0)
    wo_copy(n_kv - 1).wait()
    with jax.named_scope("project"):
        project_out((n_kv - 1) % wo_slots)
        out_v[...] = res[...].astype(BF16)

    def finish(buf, sc, sem):
        part = buf.at[:, pl.ds(2 * sc, 2)]
        pltpu.make_async_remote_copy(src_ref=part, dst_ref=part, send_sem=sem, recv_sem=far_recv.at[0, 0, 0],
                                     device_id={"sp": sibling}, device_id_type=MESH).wait_send()

    with jax.named_scope("finish_sends"):
        for t, buf in enumerate((kbuf, vbuf)):
            part = buf.at[:, me]
            pltpu.make_async_remote_copy(src_ref=part, dst_ref=part, send_sem=swap_send.at[t], recv_sem=far_recv.at[0, 0, 0],
                                         device_id={"sp": sibling}, device_id_type=MESH).wait_send()

        @pl.when((chip == 0) | ((chip + core == 1) | (chip + core == 3)) & (chip < 3))
        def _():
            finish(vbuf, 0, far_sem.at[0])

        @pl.when((chip < 2) | ((chip == 2) & (core == 1)))
        def _():
            finish(kbuf, 0, far_sem.at[1])

        @pl.when((chip == 0) & (core == 1))
        def _():
            finish(kbuf, 0, far_sem.at[2])

        @pl.when((chip >= 2) & (core == 1))
        def _():
            finish(vbuf, 0, relay_sem)
        for sc in range(chips - 1):
            @pl.when(chip > sc)
            def _():
                finish(kbuf, sc, fwd_send.at[sc])


def write_back(res_v, out_hbm, sem):
    copy = pltpu.make_async_copy(res_v, out_hbm, sem)
    copy.start()
    copy.wait()


def solution(mesh):
    def device_step(hidden, ln_gain, w_q, w_k, w_v, w_o, q_gain, k_gain):
        rows, d = hidden.shape
        hd = q_gain.shape[0]
        n_kv = w_k.shape[1] // hd
        group = w_q.shape[1] // w_k.shape[1]
        n_dev = mesh.shape['sp']
        table = jnp.asarray(rope_table(rows * n_dev, hd))
        any_spec = pl.BlockSpec(memory_space=pl.ANY)
        vmem_spec = pl.BlockSpec(memory_space=pltpu.VMEM)
        dma = pltpu.SemaphoreType.DMA
        result = pl.pallas_call(
            kernel,
            out_shape=pltpu.VMEM((rows, d), BF16),
            in_specs=[any_spec] * 9,
            out_specs=vmem_spec,
            scratch_shapes=[
                pltpu.VMEM((rows, d), BF16),
                pltpu.VMEM((rows, d), BF16),
                pltpu.VMEM((d // LANES, LANES), BF16),
                pltpu.VMEM((1, hd), BF16),
                pltpu.VMEM((1, hd), BF16),
                pltpu.VMEM((rows, hd), F32),
                pltpu.VMEM((n_kv // 2, d, 2 * hd), BF16),
                pltpu.VMEM((n_kv // 2, d, 2 * hd), BF16),
                pltpu.VMEM((5, d, group * hd), BF16),
                pltpu.VMEM((4, group * hd, d), BF16),
                pltpu.VMEM((n_kv, n_dev, rows, hd), BF16),
                pltpu.VMEM((n_kv, n_dev, hd, rows), BF16),
                pltpu.VMEM((2, rows, group * hd), F32),
                pltpu.VMEM((n_kv, group * rows, hd), BF16),
                pltpu.VMEM((hd, group * rows), BF16),
                pltpu.VMEM((rows, d), F32),
                dma((5,)),
                dma((2,)),
                dma((2,)),
                dma((5,)),
                dma((4,)),
                dma((2,)),
                dma((2, n_kv)),
                dma((3,)),
                dma((2, n_kv, n_dev // 2 - 1)),
                dma((n_dev // 2 - 1,)),
                dma,
            ],
            compiler_params=pltpu.CompilerParams(collective_id=0, has_side_effects=True, vmem_limit_bytes=62000000),
        )(hidden, ln_gain.reshape(-1, LANES), w_q, w_k, w_v, w_o, q_gain.reshape(1, -1), k_gain.reshape(1, -1), table)
        return pl.pallas_call(
            write_back,
            out_shape=jax.ShapeDtypeStruct((rows, d), BF16),
            in_specs=[vmem_spec],
            out_specs=any_spec,
            scratch_shapes=[dma],
            compiler_params=pltpu.CompilerParams(vmem_limit_bytes=1000000),
        )(result)

    row_spec = P(('dp', 'sp'), None)
    return jax.shard_map(device_step, mesh=mesh, in_specs=(row_spec, P(), P(), P(), P(), P(), P(), P()), out_specs=row_spec, check_vma=False)
```

```python
import functools

import jax
import jax.numpy as jnp
import numpy as np
from jax import lax
from jax.experimental import pallas as pl
from jax.experimental.pallas import tpu as pltpu
from jax.sharding import PartitionSpec as P

EPS = 1e-6
THETA = 1000000.0
MESH = pl.DeviceIdType.MESH
F32 = jnp.float32
BF16 = jnp.bfloat16
LANES = 128
LOG2E = 1.4426950408889634
AHEAD = 2
KV_FLIGHT = 8
K_BEHIND = 2


def rope_table(seq, head_dim):
    half = head_dim // 2
    inv_freq = np.power(np.float32(THETA), -(np.arange(half, dtype=np.float32) * np.float32(2.0 / head_dim))).astype(np.float32)
    angles = (np.arange(seq, dtype=np.float32)[:, None] * inv_freq[None, :]).astype(np.float32).astype(np.float64)
    return np.concatenate([np.cos(angles), np.sin(angles)], axis=1).astype(np.float32)


def kernel(x_hbm, ln_gain_hbm, w_q, w_k, w_v, w_o, q_gain_hbm, k_gain_hbm, tab_hbm, out_v,
           x_v, h_v, ln_gain, q_gain, k_gain, tab_v, wkv_v, wq_v, wo_v, kbuf, vbuf, qraw, qbuf, mixed_t, res, s_even, s_odd, top_even, top_odd,
           in_sem, wkv_sem, wq_sem, wo_sem,
           own_send, fwd_send, relay_send, k_recv, v_recv, v_relay):
    rows, d = x_v.shape
    n_kv, n_dev, _, hd = kbuf.shape
    group = qbuf.shape[1] // rows
    n_pairs = n_kv // 2
    wq_slots, wo_slots = wq_v.shape[0], wo_v.shape[0]
    chips = n_dev // 2
    me = lax.axis_index("sp")
    core = lax.rem(me, 2)
    chip = me // 2
    sibling = me + 1 - 2 * core
    score_scale = hd ** -0.5 * LOG2E

    x_copy = pltpu.make_async_copy(x_hbm, x_v, in_sem.at[0])
    small_copies = [
        pltpu.make_async_copy(ln_gain_hbm, ln_gain, in_sem.at[1]),
        pltpu.make_async_copy(q_gain_hbm, q_gain, in_sem.at[2]),
        pltpu.make_async_copy(k_gain_hbm, k_gain, in_sem.at[3]),
        pltpu.make_async_copy(tab_hbm.at[pl.ds(pl.multiple_of(me * rows, rows), rows)], tab_v, in_sem.at[4]),
    ]

    def kv_copies(h):
        cols = pl.ds(pl.multiple_of(h * hd, hd), hd)
        slot = lax.rem(h, KV_FLIGHT)
        return (pltpu.make_async_copy(w_k.at[:, cols], wkv_v.at[h, :, pl.ds(0, hd)], wkv_sem.at[slot]),
                pltpu.make_async_copy(w_v.at[:, cols], wkv_v.at[h, :, pl.ds(hd, hd)], wkv_sem.at[slot]))

    def kv_wait(h):
        pltpu.make_async_copy(wkv_v.at[h], wkv_v.at[h], wkv_sem.at[lax.rem(h, KV_FLIGHT)]).wait()

    def kv_start(h):
        for copy in kv_copies(h):
            copy.start()

    def wq_copy(h):
        n = group * hd
        slot = lax.rem(h, wq_slots)
        return pltpu.make_async_copy(w_q.at[:, pl.ds(pl.multiple_of(h * n, n), n)], wq_v.at[slot], wq_sem.at[slot])

    def wo_copy(h):
        n = group * hd
        slot = lax.rem(h, wo_slots)
        return pltpu.make_async_copy(w_o.at[pl.ds(pl.multiple_of(h * n, n), n)], wo_v.at[slot], wo_sem.at[slot])

    x_copy.start()
    for copy in small_copies:
        copy.start()
    kv_start(0)

    barrier = pltpu.get_barrier_semaphore()
    for step in range(1, n_dev):
        pl.semaphore_signal(barrier, inc=1, device_id={"sp": lax.rem(me + step, n_dev)}, device_id_type=MESH)

    def push(buf, h, blocks, dst, sem, recv=None):
        part = buf.at[h, blocks]
        recv = (k_recv if buf is kbuf else v_recv) if recv is None else recv
        return pltpu.make_async_remote_copy(src_ref=part, dst_ref=part, send_sem=sem, recv_sem=recv.at[h],
                                            device_id={"sp": dst}, device_id_type=MESH)

    def own(buf, h, dst, recv=None):
        push(buf, h, pl.ds(me, 1), dst, own_send.at[0 if buf is kbuf else 1], recv).start()

    def arrived(buf, h, n, recv=None):
        push(buf, h, pl.ds(0, n), sibling, own_send.at[0], recv).wait_recv()

    with jax.named_scope("gain_wait"):
        small_copies[0].wait()
    gain_rows = ln_gain[...].astype(F32)

    with jax.named_scope("x_wait"):
        x_copy.wait()
    for h in range(1, 4):
        kv_start(h)
    for r in range(0, rows, 16):
        xf = x_v[r:r + 16, :].astype(F32)
        norm = lax.rsqrt(jnp.mean(xf * xf, axis=-1, keepdims=True) + EPS)
        for c in range(d // LANES):
            cols = slice(c * LANES, (c + 1) * LANES)
            h_v[r:r + 16, cols] = (xf[:, cols] * norm * gain_rows[c:c + 1, :]).astype(BF16)

    kv_start(4)
    kv_start(5)
    with jax.named_scope("small_wait"):
        for copy in small_copies[1:]:
            copy.wait()
    table = tab_v[...]
    turned = pltpu.roll(table, hd // 2, 1)
    low = lax.broadcasted_iota(jnp.int32, table.shape, 1) < hd // 2
    cos_pos = jnp.where(low, table, turned)
    sin_pos = jnp.where(low, -turned, table)

    def head_norm_rotate(values, gain):
        gain = jnp.broadcast_to(gain[...].astype(F32), (8, hd))
        gain_turned = pltpu.roll(gain, hd // 2, 1)
        values = values * lax.rsqrt(jnp.mean(values * values, axis=-1, keepdims=True) + EPS)
        return (values * (cos_pos * gain[:1]) + pltpu.roll(values, hd // 2, 1) * (sin_pos * gain_turned[:1])).astype(BF16)

    with jax.named_scope("barrier"):
        pl.semaphore_wait(barrier, n_dev - 1)

    def on(c, k):
        return pl.when((chip == c) & (core == k))

    def send_wide(heads):
        @pl.when(chip == 0)
        def _():
            for h in heads:
                own(kbuf, h, 6)
                own(vbuf, h, 5, v_relay)
                own(vbuf, h, 3)
                own(kbuf, h, 2)

                @pl.when(h >= K_BEHIND)
                def _():
                    own(kbuf, h - K_BEHIND, 4)

        @pl.when(chip == 1)
        def _():
            for h in heads:
                own(kbuf, h, 6)
                own(vbuf, h, 7, v_relay)

    def send_near(h):
        @pl.when(chip == 2)
        def _():
            own(kbuf, h, 6)
            own(vbuf, h, 7)

    def send_transit(h):
        @pl.when(chip == 1)
        def _():
            own(kbuf, h, 4)

    def project_kv(heads):
        with jax.named_scope("wkv_wait"):
            for h in heads:
                kv_wait(h)
        with jax.named_scope("kv_step"):
            both = [jnp.dot(h_v[...], wkv_v[h], preferred_element_type=F32) for h in heads]
            for h, kv in zip(heads, both):
                kbuf[h, me] = head_norm_rotate(kv[:, :hd], k_gain)
                vbuf[h, me] = kv[:, hd:].T.astype(BF16)
        for h in heads:
            own(kbuf, h, sibling)
            own(vbuf, h, sibling)
        send_wide(heads)

    project_kv([0])
    send_near(0)
    kv_start(6)
    kv_start(7)
    project_kv([1])
    send_near(1)
    wq_copy(0).start()

    def kv_pair(p, carry):
        wq_copy(p).start()
        project_kv([2 * p, 2 * p + 1])
        return carry

    lax.fori_loop(1, n_pairs, kv_pair, 0)

    @pl.when(chip == 0)
    def _():
        for h in range(n_kv - K_BEHIND, n_kv):
            own(kbuf, h, 4)

    def q_dot(h):
        qraw[lax.rem(h, 2)] = jnp.dot(h_v[...], wq_v[lax.rem(h, wq_slots)], preferred_element_type=F32)

    def q_finish(h, slot):
        q = qraw[slot]
        for g in range(group):
            qbuf[h, g * rows:(g + 1) * rows, :] = head_norm_rotate(q[:, g * hd:(g + 1) * hd], q_gain)

    def wq_wait(h):
        with jax.named_scope("wq_wait"):
            wq_copy(h).wait()

    def relay(h, c):
        @pl.when((chip == c) & (core == 1))
        @jax.named_scope("relay")
        def _():
            blocks = pl.ds(2 * (c - 2), 2)
            arrived(vbuf, h, 2, v_relay)
            push(vbuf, h, blocks, sibling, fwd_send).start()
            push(vbuf, h, blocks, 11 - 2 * c, relay_send).start()

    def direct_k(h):
        for c in range(chips):
            @pl.when((chip == c) & (core == 0))
            @jax.named_scope("direct_k")
            def _():
                arrived(kbuf, h, 2 * c + 1)
                if c:
                    push(kbuf, h, pl.ds(0, 2 * c), sibling, fwd_send).start()

    def direct_v(h):
        for c in range(chips):
            @pl.when((chip == c) & (core == 1))
            @jax.named_scope("direct_v")
            def _():
                if c < 2:
                    arrived(vbuf, h, 2 * c + 1)
                    if c:
                        push(vbuf, h, pl.ds(0, 2), sibling, fwd_send).start()
                elif c == 2:
                    arrived(vbuf, h, 3)
                    push(vbuf, h, pl.ds(2, 2), sibling, fwd_send).start()
                else:
                    arrived(vbuf, h, 5)
                    push(vbuf, h, pl.ds(0, 2), sibling, fwd_send).start()
                    push(vbuf, h, pl.ds(4, 2), sibling, fwd_send).start()

    def wait_k(h, c):
        @pl.when(core == 1)
        @jax.named_scope("wait_k")
        def _():
            arrived(kbuf, h, 2 * c + 1)

    def wait_v(h, c):
        @pl.when(core == 0)
        @jax.named_scope("wait_v")
        def _():
            arrived(vbuf, h, 2 * c + 1)

    def make_scores(h, c, s_out, top_out):
        n_keys = 2 * (c + 1) * rows
        keys = kbuf[h, 0:2 * (c + 1)].reshape(n_keys, hd)
        key_id = lax.broadcasted_iota(jnp.int32, (2 * rows, rows), 0)
        row_id = lax.broadcasted_iota(jnp.int32, (2 * rows, rows), 1)
        visible = jnp.concatenate([key_id <= row_id + core * rows] * group, axis=1)
        scores = lax.dot_general(keys, qbuf[h], (((1,), (1,)), ((), ())), preferred_element_type=F32)
        last = jnp.where(visible, scores[n_keys - 2 * rows:], -jnp.inf)
        scores = jnp.concatenate([scores[:n_keys - 2 * rows], last], axis=0) if c else last
        s_out[0:n_keys, :] = scores
        top_out[...] = jnp.broadcast_to(jnp.max(scores, axis=0, keepdims=True), top_out.shape)

    def mix(h, c, s_in, top_in):
        n_keys = 2 * (c + 1) * rows
        vals = jnp.concatenate([vbuf[h, src] for src in range(2 * (c + 1))], axis=1)
        probs = jnp.exp2((s_in[0:n_keys, :] - top_in[0:1, :]) * score_scale)
        total = jnp.sum(probs, axis=0, keepdims=True)
        mixed = jnp.dot(vals, probs.astype(BF16), preferred_element_type=F32)
        mixed_t[...] = (mixed / total).astype(BF16)

    def project_out(slot):
        mixed = jnp.concatenate([mixed_t[:, g * rows:(g + 1) * rows].T for g in range(group)], axis=1)
        res[...] += jnp.dot(mixed, wo_v[slot], preferred_element_type=F32)

    def relay_step(h):
        relay(h, 2)

        @pl.when(h + AHEAD < n_kv)
        def _():
            send_near(h + AHEAD)
        send_transit(h)

    def q_step(h, carry):
        wq_wait(h)

        @pl.when(h < n_kv - 4)
        def _():
            wq_copy(h + 4).start()

        @pl.when(h >= n_kv - 4)
        def _():
            wo_copy(h - (n_kv - 4)).start()

        with jax.named_scope("q_step"):
            q_finish(jnp.maximum(h - 1, 0), lax.rem(h + 1, 2))
            q_dot(h)
            some = pl.ds(pl.multiple_of(h * 16, 16), 16)
            res[some, :] = x_v[some, :].astype(F32)

        @pl.when(h == 0)
        def _():
            relay_step(0)

        @pl.when(lax.rem(h, 3) == 1)
        def _():
            relay_step(h // 3 + 1)

        @pl.when((h == n_kv - 5) | (h == n_kv - 3))
        def _():
            relay(h // 2 - 1, 3)
            direct_k(h // 2 - 1)

        @pl.when(h == n_kv - 2)
        def _():
            direct_v(0)
        return carry

    lax.fori_loop(0, n_kv, q_step, 0)
    with jax.named_scope("wo_wait"):
        wo_copy(0).wait()
    mixed_t[...] = jnp.zeros_like(mixed_t)

    for c in range(chips):
        @pl.when(chip == c)
        def _():
            wait_k(0, c)
            with jax.named_scope("first_scores"):
                make_scores(0, c, s_even, top_even)
                q_finish(n_kv - 1, (n_kv - 1) % 2)

    def head_step(h, this, other, tail):
        @pl.when(h < n_kv - 2)
        def _():
            direct_k(h + 2)
            relay(h + 2, 3)
            direct_v(h + 1)

        @pl.when(h > 1)
        @jax.named_scope("wo_wait")
        def _():
            wo_copy(h - 1).wait()

        for c in range(chips):
            @pl.when(chip == c)
            def _():
                def block(more):
                    wait_v(h, c)
                    if more:
                        wait_k(h + 1, c)
                    with jax.named_scope("attend"):
                        if more:
                            project_out(lax.rem(jnp.maximum(h - 1, 0), wo_slots))
                            make_scores(h + 1, c, *other)
                        mix(h, c, *this)

                if not tail:
                    block(True)
                else:
                    @pl.when(h < n_kv - 1)
                    def _():
                        block(True)

                    @pl.when(h == n_kv - 1)
                    def _():
                        with jax.named_scope("project"):
                            project_out((n_kv - 2) % wo_slots)
                        block(False)

        if not tail:
            @pl.when(h == n_kv - 2)
            def _():
                direct_v(n_kv - 1)

        @pl.when((h > 0) & (h < n_kv - 3))
        def _():
            wo_copy(h + 3).start()

        @pl.when(h < n_kv - 4)
        def _():
            relay_step(h + 4)

    def two_heads(i, carry):
        head_step(2 * i, (s_even, top_even), (s_odd, top_odd), False)
        head_step(2 * i + 1, (s_odd, top_odd), (s_even, top_even), True)
        return carry

    lax.fori_loop(0, n_kv // 2, two_heads, 0)
    wo_copy(n_kv - 1).wait()
    with jax.named_scope("project"):
        project_out((n_kv - 1) % wo_slots)
        out_v[...] = res[...].astype(BF16)

    def sent(buf, heads, blocks, sem):
        part = buf.at[0:heads, 0:blocks]
        pltpu.make_async_remote_copy(src_ref=part, dst_ref=part, send_sem=sem, recv_sem=k_recv.at[0],
                                     device_id={"sp": sibling}, device_id_type=MESH).wait_send()

    with jax.named_scope("finish_sends"):
        for c in range(chips):
            @pl.when(chip == c)
            def _():
                sent(kbuf, n_kv, (4, 3, 2, 1)[c], own_send.at[0])
                sent(vbuf, n_kv, (3, 2, 2, 1)[c], own_send.at[1])
                if c:
                    sent(kbuf, n_kv, 2 * c, fwd_send)
                if c >= 2:
                    @pl.when(core == 1)
                    def _():
                        sent(vbuf, n_kv, 2, relay_send)


def write_back(res_v, out_hbm, sem):
    copy = pltpu.make_async_copy(res_v, out_hbm, sem)
    copy.start()
    copy.wait()


def solution(mesh):
    def device_step(hidden, ln_gain, w_q, w_k, w_v, w_o, q_gain, k_gain):
        rows, d = hidden.shape
        hd = q_gain.shape[0]
        n_kv = w_k.shape[1] // hd
        group = w_q.shape[1] // w_k.shape[1]
        n_dev = mesh.shape['sp']
        table = jnp.asarray(rope_table(rows * n_dev, hd))
        any_spec = pl.BlockSpec(memory_space=pl.ANY)
        vmem_spec = pl.BlockSpec(memory_space=pltpu.VMEM)
        dma = pltpu.SemaphoreType.DMA
        result = pl.pallas_call(
            kernel,
            out_shape=pltpu.VMEM((rows, d), BF16),
            in_specs=[any_spec] * 9,
            out_specs=vmem_spec,
            scratch_shapes=[
                pltpu.VMEM((rows, d), BF16),
                pltpu.VMEM((rows, d), BF16),
                pltpu.VMEM((d // LANES, LANES), BF16),
                pltpu.VMEM((1, hd), BF16),
                pltpu.VMEM((1, hd), BF16),
                pltpu.VMEM((rows, hd), F32),
                pltpu.VMEM((n_kv, d, 2 * hd), BF16),
                pltpu.VMEM((5, d, group * hd), BF16),
                pltpu.VMEM((4, group * hd, d), BF16),
                pltpu.VMEM((n_kv, n_dev, rows, hd), BF16),
                pltpu.VMEM((n_kv, n_dev, hd, rows), BF16),
                pltpu.VMEM((2, rows, group * hd), F32),
                pltpu.VMEM((n_kv, group * rows, hd), BF16),
                pltpu.VMEM((hd, group * rows), BF16),
                pltpu.VMEM((rows, d), F32),
                pltpu.VMEM((rows * n_dev, group * rows), F32),
                pltpu.VMEM((rows * n_dev, group * rows), F32),
                pltpu.VMEM((8, group * rows), F32),
                pltpu.VMEM((8, group * rows), F32),
                dma((5,)),
                dma((KV_FLIGHT,)),
                dma((5,)),
                dma((4,)),
                dma((2,)),
                dma,
                dma,
                dma((n_kv,)),
                dma((n_kv,)),
                dma((n_kv,)),
            ],
            compiler_params=pltpu.CompilerParams(collective_id=0, has_side_effects=True, vmem_limit_bytes=62000000),
        )(hidden, ln_gain.reshape(-1, LANES), w_q, w_k, w_v, w_o, q_gain.reshape(1, -1), k_gain.reshape(1, -1), table)
        return pl.pallas_call(
            write_back,
            out_shape=jax.ShapeDtypeStruct((rows, d), BF16),
            in_specs=[vmem_spec],
            out_specs=any_spec,
            scratch_shapes=[dma],
            compiler_params=pltpu.CompilerParams(vmem_limit_bytes=1000000),
        )(result)

    row_spec = P(('dp', 'sp'), None)
    return jax.shard_map(device_step, mesh=mesh, in_specs=(row_spec, P(), P(), P(), P(), P(), P(), P()), out_specs=row_spec, check_vma=False)
```

```python
import functools

import jax
import jax.numpy as jnp
import numpy as np
from jax import lax
from jax.experimental import pallas as pl
from jax.experimental.pallas import tpu as pltpu
from jax.sharding import PartitionSpec as P

EPS = 1e-6
THETA = 1000000.0
MESH = pl.DeviceIdType.MESH
F32 = jnp.float32
BF16 = jnp.bfloat16
LANES = 128
LOG2E = 1.4426950408889634
AHEAD = 2
KV_FLIGHT = 8
K_BEHIND = 2


def rope_table(seq, head_dim):
    half = head_dim // 2
    inv_freq = np.power(np.float32(THETA), -(np.arange(half, dtype=np.float32) * np.float32(2.0 / head_dim))).astype(np.float32)
    angles = (np.arange(seq, dtype=np.float32)[:, None] * inv_freq[None, :]).astype(np.float32).astype(np.float64)
    return np.concatenate([np.cos(angles), np.sin(angles)], axis=1).astype(np.float32)


def kernel(x_hbm, ln_gain_hbm, w_q, w_k, w_v, w_o, q_gain_hbm, k_gain_hbm, tab_hbm, out_v,
           x_v, h_v, ln_gain, q_gain, k_gain, tab_v, wkv_v, wq_v, wo_v, kbuf, vbuf, qraw, qbuf, mixed_t, res, s_even, s_odd, top_even, top_odd,
           in_sem, wkv_sem, wq_sem, wo_sem,
           own_send, fwd_send, relay_send, k_recv, v_recv, v_relay):
    rows, d = x_v.shape
    n_kv, n_dev, _, hd = kbuf.shape
    group = qbuf.shape[1] // rows
    n_pairs = n_kv // 2
    wq_slots, wo_slots = wq_v.shape[0], wo_v.shape[0]
    chips = n_dev // 2
    me = lax.axis_index("sp")
    core = lax.rem(me, 2)
    chip = me // 2
    sibling = me + 1 - 2 * core
    score_scale = hd ** -0.5 * LOG2E

    x_copy = pltpu.make_async_copy(x_hbm, x_v, in_sem.at[0])
    small_copies = [
        pltpu.make_async_copy(ln_gain_hbm, ln_gain, in_sem.at[1]),
        pltpu.make_async_copy(q_gain_hbm, q_gain, in_sem.at[2]),
        pltpu.make_async_copy(k_gain_hbm, k_gain, in_sem.at[3]),
        pltpu.make_async_copy(tab_hbm.at[pl.ds(pl.multiple_of(me * rows, rows), rows)], tab_v, in_sem.at[4]),
    ]

    def kv_copies(h):
        cols = pl.ds(pl.multiple_of(h * hd, hd), hd)
        slot = lax.rem(h, KV_FLIGHT)
        return (pltpu.make_async_copy(w_k.at[:, cols], wkv_v.at[h, :, pl.ds(0, hd)], wkv_sem.at[slot]),
                pltpu.make_async_copy(w_v.at[:, cols], wkv_v.at[h, :, pl.ds(hd, hd)], wkv_sem.at[slot]))

    def kv_wait(h):
        pltpu.make_async_copy(wkv_v.at[h], wkv_v.at[h], wkv_sem.at[lax.rem(h, KV_FLIGHT)]).wait()

    def kv_start(h):
        for copy in kv_copies(h):
            copy.start()

    def wq_copy(h):
        n = group * hd
        slot = lax.rem(h, wq_slots)
        return pltpu.make_async_copy(w_q.at[:, pl.ds(pl.multiple_of(h * n, n), n)], wq_v.at[slot], wq_sem.at[slot])

    def wo_copy(h):
        n = group * hd
        slot = lax.rem(h, wo_slots)
        return pltpu.make_async_copy(w_o.at[pl.ds(pl.multiple_of(h * n, n), n)], wo_v.at[slot], wo_sem.at[slot])

    x_copy.start()
    for copy in small_copies:
        copy.start()
    kv_start(0)

    barrier = pltpu.get_barrier_semaphore()
    for step in range(1, n_dev):
        pl.semaphore_signal(barrier, inc=1, device_id={"sp": lax.rem(me + step, n_dev)}, device_id_type=MESH)

    def push(buf, h, blocks, dst, sem, recv=None):
        part = buf.at[h, blocks]
        recv = (k_recv if buf is kbuf else v_recv) if recv is None else recv
        return pltpu.make_async_remote_copy(src_ref=part, dst_ref=part, send_sem=sem, recv_sem=recv.at[h],
                                            device_id={"sp": dst}, device_id_type=MESH)

    def own(buf, h, dst, recv=None):
        push(buf, h, pl.ds(me, 1), dst, own_send.at[0 if buf is kbuf else 1], recv).start()

    def arrived(buf, h, n, recv=None):
        push(buf, h, pl.ds(0, n), sibling, own_send.at[0], recv).wait_recv()

    with jax.named_scope("gain_wait"):
        small_copies[0].wait()
    gain_rows = ln_gain[...].astype(F32)

    with jax.named_scope("x_wait"):
        x_copy.wait()
    for h in range(1, 4):
        kv_start(h)
    for r in range(0, rows, 16):
        xf = x_v[r:r + 16, :].astype(F32)
        norm = lax.rsqrt(jnp.mean(xf * xf, axis=-1, keepdims=True) + EPS)
        for c in range(d // LANES):
            cols = slice(c * LANES, (c + 1) * LANES)
            h_v[r:r + 16, cols] = (xf[:, cols] * norm * gain_rows[c:c + 1, :]).astype(BF16)

    kv_start(4)
    kv_start(5)
    with jax.named_scope("small_wait"):
        for copy in small_copies[1:]:
            copy.wait()
    table = tab_v[...]
    turned = pltpu.roll(table, hd // 2, 1)
    low = lax.broadcasted_iota(jnp.int32, table.shape, 1) < hd // 2
    cos_pos = jnp.where(low, table, turned)
    sin_pos = jnp.where(low, -turned, table)

    def head_norm_rotate(values, gain):
        gain = jnp.broadcast_to(gain[...].astype(F32), (8, hd))
        gain_turned = pltpu.roll(gain, hd // 2, 1)
        values = values * lax.rsqrt(jnp.mean(values * values, axis=-1, keepdims=True) + EPS)
        return (values * (cos_pos * gain[:1]) + pltpu.roll(values, hd // 2, 1) * (sin_pos * gain_turned[:1])).astype(BF16)

    with jax.named_scope("barrier"):
        pl.semaphore_wait(barrier, n_dev - 1)

    def on(c, k):
        return pl.when((chip == c) & (core == k))

    def send_wide(heads):
        @pl.when(chip == 0)
        def _():
            for h in heads:
                own(kbuf, h, 6)
                own(vbuf, h, 5, v_relay)
                own(vbuf, h, 3)
                own(kbuf, h, 2)

                @pl.when(h >= K_BEHIND)
                def _():
                    own(kbuf, h - K_BEHIND, 4)

        @pl.when(chip == 1)
        def _():
            for h in heads:
                own(vbuf, h, 7, v_relay)
                own(kbuf, h, 6)

    def send_near(h):
        @pl.when(chip == 2)
        def _():
            own(kbuf, h, 6)
            own(vbuf, h, 7)

    def send_transit(h):
        @pl.when(chip == 1)
        def _():
            own(kbuf, h, 4)

    def project_kv(heads):
        with jax.named_scope("wkv_wait"):
            for h in heads:
                kv_wait(h)
        with jax.named_scope("kv_step"):
            both = [jnp.dot(h_v[...], wkv_v[h], preferred_element_type=F32) for h in heads]
            for h, kv in zip(heads, both):
                kbuf[h, me] = head_norm_rotate(kv[:, :hd], k_gain)
                vbuf[h, me] = kv[:, hd:].T.astype(BF16)
        for h in heads:
            own(kbuf, h, sibling)
            own(vbuf, h, sibling)
        send_wide(heads)

    project_kv([0])
    send_near(0)
    kv_start(6)
    kv_start(7)
    project_kv([1])
    send_near(1)
    wq_copy(0).start()

    def kv_pair(p, carry):
        wq_copy(p).start()
        project_kv([2 * p, 2 * p + 1])
        return carry

    lax.fori_loop(1, n_pairs, kv_pair, 0)

    @pl.when(chip == 0)
    def _():
        for h in range(n_kv - K_BEHIND, n_kv):
            own(kbuf, h, 4)

    def q_dot(h):
        qraw[lax.rem(h, 2)] = jnp.dot(h_v[...], wq_v[lax.rem(h, wq_slots)], preferred_element_type=F32)

    def q_finish(h, slot):
        q = qraw[slot]
        for g in range(group):
            qbuf[h, g * rows:(g + 1) * rows, :] = head_norm_rotate(q[:, g * hd:(g + 1) * hd], q_gain)

    def wq_wait(h):
        with jax.named_scope("wq_wait"):
            wq_copy(h).wait()

    def relay(h, c):
        @pl.when((chip == c) & (core == 1))
        @jax.named_scope("relay")
        def _():
            blocks = pl.ds(2 * (c - 2), 2)
            arrived(vbuf, h, 2, v_relay)
            push(vbuf, h, blocks, sibling, fwd_send).start()
            push(vbuf, h, blocks, 11 - 2 * c, relay_send).start()
            if c == 3:
                push(vbuf, h, blocks, 4, relay_send).start()

    def direct_k(h):
        for c in range(chips):
            @pl.when((chip == c) & (core == 0))
            @jax.named_scope("direct_k")
            def _():
                arrived(kbuf, h, 2 * c + 1)
                if c:
                    push(kbuf, h, pl.ds(0, 2 * c), sibling, fwd_send).start()

    def direct_v(h, those=range(4)):
        for c in those:
            @pl.when((chip == c) & (core == 1))
            @jax.named_scope("direct_v")
            def _():
                if c < 2:
                    arrived(vbuf, h, 2 * c + 1)
                    if c:
                        push(vbuf, h, pl.ds(0, 2), sibling, fwd_send).start()
                elif c == 3:
                    arrived(vbuf, h, 5)
                    push(vbuf, h, pl.ds(0, 2), sibling, fwd_send).start()
                    push(vbuf, h, pl.ds(4, 2), sibling, fwd_send).start()

    def wait_k(h, c):
        @pl.when(core == 1)
        @jax.named_scope("wait_k")
        def _():
            arrived(kbuf, h, 2 * c + 1)

    def wait_v(h, c):
        @pl.when(core == 0)
        @jax.named_scope("wait_v")
        def _():
            arrived(vbuf, h, 2 * c + 1)

        if c == 2:
            @pl.when(core == 1)
            @jax.named_scope("wait_v")
            def _():
                arrived(vbuf, h, 3)

    def make_scores(h, c, s_out, top_out):
        n_keys = 2 * (c + 1) * rows
        keys = kbuf[h, 0:2 * (c + 1)].reshape(n_keys, hd)
        key_id = lax.broadcasted_iota(jnp.int32, (2 * rows, rows), 0)
        row_id = lax.broadcasted_iota(jnp.int32, (2 * rows, rows), 1)
        visible = jnp.concatenate([key_id <= row_id + core * rows] * group, axis=1)
        scores = lax.dot_general(keys, qbuf[h], (((1,), (1,)), ((), ())), preferred_element_type=F32)
        last = jnp.where(visible, scores[n_keys - 2 * rows:], -jnp.inf)
        scores = jnp.concatenate([scores[:n_keys - 2 * rows], last], axis=0) if c else last
        s_out[0:n_keys, :] = scores
        top_out[...] = jnp.broadcast_to(jnp.max(scores, axis=0, keepdims=True), top_out.shape)

    def mix(h, c, s_in, top_in):
        n_keys = 2 * (c + 1) * rows
        vals = jnp.concatenate([vbuf[h, src] for src in range(2 * (c + 1))], axis=1)
        probs = jnp.exp2((s_in[0:n_keys, :] - top_in[0:1, :]) * score_scale)
        total = jnp.sum(probs, axis=0, keepdims=True)
        mixed = jnp.dot(vals, probs.astype(BF16), preferred_element_type=F32)
        mixed_t[...] = (mixed / total).astype(BF16)

    def project_out(slot):
        mixed = jnp.concatenate([mixed_t[:, g * rows:(g + 1) * rows].T for g in range(group)], axis=1)
        res[...] += jnp.dot(mixed, wo_v[slot], preferred_element_type=F32)

    def relay_step(h):
        relay(h, 2)

        @pl.when(h + AHEAD < n_kv)
        def _():
            send_near(h + AHEAD)
        send_transit(h)

    def q_step(h, carry):
        wq_wait(h)

        @pl.when(h < n_kv - 4)
        def _():
            wq_copy(h + 4).start()

        @pl.when(h >= n_kv - 4)
        def _():
            wo_copy(h - (n_kv - 4)).start()

        with jax.named_scope("q_step"):
            q_finish(jnp.maximum(h - 1, 0), lax.rem(h + 1, 2))
            q_dot(h)
            some = pl.ds(pl.multiple_of(h * 16, 16), 16)
            res[some, :] = x_v[some, :].astype(F32)

        @pl.when(h == 0)
        def _():
            relay_step(0)

        @pl.when(lax.rem(h, 3) == 1)
        def _():
            relay_step(h // 3 + 1)

        @pl.when((h == n_kv - 5) | (h == n_kv - 3) | (h == n_kv - 1))
        def _():
            relay(h // 2 - 1, 3)

        @pl.when((h == n_kv - 5) | (h == n_kv - 3))
        def _():
            direct_k(h // 2 - 1)

        @pl.when(h == n_kv - 2)
        def _():
            direct_v(0)
        return carry

    lax.fori_loop(0, n_kv, q_step, 0)
    with jax.named_scope("wo_wait"):
        wo_copy(0).wait()
    mixed_t[...] = jnp.zeros_like(mixed_t)

    for c in range(chips):
        @pl.when(chip == c)
        def _():
            wait_k(0, c)
            with jax.named_scope("first_scores"):
                make_scores(0, c, s_even, top_even)
                q_finish(n_kv - 1, (n_kv - 1) % 2)

    def head_step(h, this, other, tail):
        @pl.when(h < n_kv - 2)
        def _():
            direct_k(h + 2)

        @pl.when((h > 0) & (h < n_kv - 2))
        def _():
            relay(h + 2, 3)

        @pl.when(h < n_kv - 2)
        def _():
            direct_v(h + 1, range(chips - 1))

        @pl.when(h < n_kv - 1)
        def _():
            direct_v(h + 1, [chips - 1])

        @pl.when(h > 1)
        @jax.named_scope("wo_wait")
        def _():
            wo_copy(h - 1).wait()

        for c in range(chips):
            @pl.when(chip == c)
            def _():
                def block(more):
                    wait_v(h, c)
                    if more:
                        wait_k(h + 1, c)
                    with jax.named_scope("attend"):
                        if more:
                            project_out(lax.rem(jnp.maximum(h - 1, 0), wo_slots))
                            make_scores(h + 1, c, *other)
                        mix(h, c, *this)

                if not tail:
                    block(True)
                else:
                    @pl.when(h < n_kv - 1)
                    def _():
                        block(True)

                    @pl.when(h == n_kv - 1)
                    def _():
                        if c >= chips - 2:
                            wait_v(h, c)
                            with jax.named_scope("attend"):
                                project_out((n_kv - 2) % wo_slots)
                                mix(h, c, *this)
                        else:
                            with jax.named_scope("project"):
                                project_out((n_kv - 2) % wo_slots)
                            block(False)

        if not tail:
            @pl.when(h == n_kv - 2)
            def _():
                direct_v(n_kv - 1, range(chips - 1))

        @pl.when((h > 0) & (h < n_kv - 3))
        def _():
            wo_copy(h + 3).start()

        @pl.when(h < n_kv - 4)
        def _():
            relay_step(h + 4)

    def two_heads(i, carry):
        head_step(2 * i, (s_even, top_even), (s_odd, top_odd), False)
        head_step(2 * i + 1, (s_odd, top_odd), (s_even, top_even), True)
        return carry

    lax.fori_loop(0, n_kv // 2, two_heads, 0)
    wo_copy(n_kv - 1).wait()
    with jax.named_scope("project"):
        project_out((n_kv - 1) % wo_slots)
        out_v[...] = res[...].astype(BF16)

    def sent(buf, heads, blocks, sem):
        part = buf.at[0:heads, 0:blocks]
        pltpu.make_async_remote_copy(src_ref=part, dst_ref=part, send_sem=sem, recv_sem=k_recv.at[0],
                                     device_id={"sp": sibling}, device_id_type=MESH).wait_send()

    with jax.named_scope("finish_sends"):
        for c in range(chips):
            @pl.when(chip == c)
            def _():
                sent(kbuf, n_kv, (4, 3, 2, 1)[c], own_send.at[0])
                sent(vbuf, n_kv, (3, 2, 2, 1)[c], own_send.at[1])
                if c in (1, 3):
                    sent(kbuf, n_kv, 2 * c, fwd_send)
                if c == 2:
                    @pl.when(core == 0)
                    def _():
                        sent(kbuf, n_kv, 4, fwd_send)

                    @pl.when(core == 1)
                    def _():
                        sent(vbuf, n_kv, 2, fwd_send)
                        sent(vbuf, n_kv, 2, relay_send)
                if c == 3:
                    @pl.when(core == 1)
                    def _():
                        sent(vbuf, n_kv, 4, relay_send)


def write_back(res_v, out_hbm, sem):
    copy = pltpu.make_async_copy(res_v, out_hbm, sem)
    copy.start()
    copy.wait()


def solution(mesh):
    def device_step(hidden, ln_gain, w_q, w_k, w_v, w_o, q_gain, k_gain):
        rows, d = hidden.shape
        hd = q_gain.shape[0]
        n_kv = w_k.shape[1] // hd
        group = w_q.shape[1] // w_k.shape[1]
        n_dev = mesh.shape['sp']
        table = jnp.asarray(rope_table(rows * n_dev, hd))
        any_spec = pl.BlockSpec(memory_space=pl.ANY)
        vmem_spec = pl.BlockSpec(memory_space=pltpu.VMEM)
        dma = pltpu.SemaphoreType.DMA
        result = pl.pallas_call(
            kernel,
            out_shape=pltpu.VMEM((rows, d), BF16),
            in_specs=[any_spec] * 9,
            out_specs=vmem_spec,
            scratch_shapes=[
                pltpu.VMEM((rows, d), BF16),
                pltpu.VMEM((rows, d), BF16),
                pltpu.VMEM((d // LANES, LANES), BF16),
                pltpu.VMEM((1, hd), BF16),
                pltpu.VMEM((1, hd), BF16),
                pltpu.VMEM((rows, hd), F32),
                pltpu.VMEM((n_kv, d, 2 * hd), BF16),
                pltpu.VMEM((5, d, group * hd), BF16),
                pltpu.VMEM((4, group * hd, d), BF16),
                pltpu.VMEM((n_kv, n_dev, rows, hd), BF16),
                pltpu.VMEM((n_kv, n_dev, hd, rows), BF16),
                pltpu.VMEM((2, rows, group * hd), F32),
                pltpu.VMEM((n_kv, group * rows, hd), BF16),
                pltpu.VMEM((hd, group * rows), BF16),
                pltpu.VMEM((rows, d), F32),
                pltpu.VMEM((rows * n_dev, group * rows), F32),
                pltpu.VMEM((rows * n_dev, group * rows), F32),
                pltpu.VMEM((8, group * rows), F32),
                pltpu.VMEM((8, group * rows), F32),
                dma((5,)),
                dma((KV_FLIGHT,)),
                dma((5,)),
                dma((4,)),
                dma((2,)),
                dma,
                dma,
                dma((n_kv,)),
                dma((n_kv,)),
                dma((n_kv,)),
            ],
            compiler_params=pltpu.CompilerParams(collective_id=0, has_side_effects=True, vmem_limit_bytes=62000000),
        )(hidden, ln_gain.reshape(-1, LANES), w_q, w_k, w_v, w_o, q_gain.reshape(1, -1), k_gain.reshape(1, -1), table)
        return pl.pallas_call(
            write_back,
            out_shape=jax.ShapeDtypeStruct((rows, d), BF16),
            in_specs=[vmem_spec],
            out_specs=any_spec,
            scratch_shapes=[dma],
            compiler_params=pltpu.CompilerParams(vmem_limit_bytes=1000000),
        )(result)

    row_spec = P(('dp', 'sp'), None)
    return jax.shard_map(device_step, mesh=mesh, in_specs=(row_spec, P(), P(), P(), P(), P(), P(), P()), out_specs=row_spec, check_vma=False)
```

```python
import functools

import jax
import jax.numpy as jnp
import numpy as np
from jax import lax
from jax.experimental import pallas as pl
from jax.experimental.pallas import tpu as pltpu
from jax.sharding import PartitionSpec as P

EPS = 1e-6
THETA = 1000000.0
MESH = pl.DeviceIdType.MESH
F32 = jnp.float32
BF16 = jnp.bfloat16
LANES = 128
LOG2E = 1.4426950408889634
AHEAD = 2
KV_FLIGHT = 8
K_BEHIND = 2


def rope_table(seq, head_dim):
    half = head_dim // 2
    inv_freq = np.power(np.float32(THETA), -(np.arange(half, dtype=np.float32) * np.float32(2.0 / head_dim))).astype(np.float32)
    angles = (np.arange(seq, dtype=np.float32)[:, None] * inv_freq[None, :]).astype(np.float32).astype(np.float64)
    return np.concatenate([np.cos(angles), np.sin(angles)], axis=1).astype(np.float32)


def kernel(x_hbm, ln_gain_hbm, w_q, w_k, w_v, w_o, q_gain_hbm, k_gain_hbm, tab_hbm, out_v,
           x_v, h_v, ln_gain, q_gain, k_gain, tab_v, wkv_v, wq_v, wo_v, kbuf, vbuf, qraw, qbuf, mixed_t, res, s_even, s_odd, top_even, top_odd,
           in_sem, wkv_sem, wq_sem, wo_sem,
           own_send, fwd_send, relay_send, k_recv, v_recv, v_relay):
    rows, d = x_v.shape
    n_kv, n_dev, _, hd = kbuf.shape
    group = qbuf.shape[1] // rows
    n_pairs = n_kv // 2
    wq_slots, wo_slots = wq_v.shape[0], wo_v.shape[0]
    chips = n_dev // 2
    me = lax.axis_index("sp")
    core = lax.rem(me, 2)
    chip = me // 2
    sibling = me + 1 - 2 * core
    score_scale = hd ** -0.5 * LOG2E

    x_copy = pltpu.make_async_copy(x_hbm, x_v, in_sem.at[0])
    small_copies = [
        pltpu.make_async_copy(ln_gain_hbm, ln_gain, in_sem.at[1]),
        pltpu.make_async_copy(q_gain_hbm, q_gain, in_sem.at[2]),
        pltpu.make_async_copy(k_gain_hbm, k_gain, in_sem.at[3]),
        pltpu.make_async_copy(tab_hbm.at[pl.ds(pl.multiple_of(me * rows, rows), rows)], tab_v, in_sem.at[4]),
    ]

    def kv_copies(h):
        cols = pl.ds(pl.multiple_of(h * hd, hd), hd)
        slot = lax.rem(h, KV_FLIGHT)
        return (pltpu.make_async_copy(w_k.at[:, cols], wkv_v.at[h, :, pl.ds(0, hd)], wkv_sem.at[slot]),
                pltpu.make_async_copy(w_v.at[:, cols], wkv_v.at[h, :, pl.ds(hd, hd)], wkv_sem.at[slot]))

    def kv_wait(h):
        pltpu.make_async_copy(wkv_v.at[h], wkv_v.at[h], wkv_sem.at[lax.rem(h, KV_FLIGHT)]).wait()

    def kv_start(h):
        for copy in kv_copies(h):
            copy.start()

    def wq_copy(h):
        n = group * hd
        slot = lax.rem(h, wq_slots)
        return pltpu.make_async_copy(w_q.at[:, pl.ds(pl.multiple_of(h * n, n), n)], wq_v.at[slot], wq_sem.at[slot])

    def wo_copy(h):
        n = group * hd
        slot = lax.rem(h, wo_slots)
        return pltpu.make_async_copy(w_o.at[pl.ds(pl.multiple_of(h * n, n), n)], wo_v.at[slot], wo_sem.at[slot])

    small_copies[0].start()
    x_copy.start()
    small_copies[3].start()
    for copy in small_copies[1:3]:
        copy.start()
    kv_start(0)

    barrier = pltpu.get_barrier_semaphore()
    for step in range(1, n_dev):
        pl.semaphore_signal(barrier, inc=1, device_id={"sp": lax.rem(me + step, n_dev)}, device_id_type=MESH)

    def push(buf, h, blocks, dst, sem, recv=None):
        part = buf.at[h, blocks]
        recv = (k_recv if buf is kbuf else v_recv) if recv is None else recv
        return pltpu.make_async_remote_copy(src_ref=part, dst_ref=part, send_sem=sem, recv_sem=recv.at[h],
                                            device_id={"sp": dst}, device_id_type=MESH)

    def own(buf, h, dst, recv=None):
        push(buf, h, pl.ds(me, 1), dst, own_send.at[0 if buf is kbuf else 1], recv).start()

    def arrived(buf, h, n, recv=None):
        push(buf, h, pl.ds(0, n), sibling, own_send.at[0], recv).wait_recv()

    with jax.named_scope("gain_wait"):
        small_copies[0].wait()
    gain_rows = ln_gain[...].astype(F32)

    with jax.named_scope("x_wait"):
        x_copy.wait()
    for h in range(1, 4):
        kv_start(h)
    for r in range(0, rows, 16):
        xf = x_v[r:r + 16, :].astype(F32)
        norm = lax.rsqrt(jnp.mean(xf * xf, axis=-1, keepdims=True) + EPS)
        for c in range(d // LANES):
            cols = slice(c * LANES, (c + 1) * LANES)
            h_v[r:r + 16, cols] = (xf[:, cols] * norm * gain_rows[c:c + 1, :]).astype(BF16)

    kv_start(4)
    kv_start(5)
    with jax.named_scope("small_wait"):
        for copy in small_copies[1:]:
            copy.wait()
    table = tab_v[...]
    turned = pltpu.roll(table, hd // 2, 1)
    low = lax.broadcasted_iota(jnp.int32, table.shape, 1) < hd // 2
    cos_pos = jnp.where(low, table, turned)
    sin_pos = jnp.where(low, -turned, table)

    def head_norm_rotate(values, gain):
        gain = jnp.broadcast_to(gain[...].astype(F32), (8, hd))
        gain_turned = pltpu.roll(gain, hd // 2, 1)
        values = values * lax.rsqrt(jnp.mean(values * values, axis=-1, keepdims=True) + EPS)
        return (values * (cos_pos * gain[:1]) + pltpu.roll(values, hd // 2, 1) * (sin_pos * gain_turned[:1])).astype(BF16)

    with jax.named_scope("barrier"):
        pl.semaphore_wait(barrier, n_dev - 1)

    def on(c, k):
        return pl.when((chip == c) & (core == k))

    def send_wide(heads):
        @pl.when(chip == 0)
        def _():
            for h in heads:
                own(kbuf, h, 6)
                own(vbuf, h, 5, v_relay)
                own(vbuf, h, 3)
                own(kbuf, h, 2)

                @pl.when(h >= K_BEHIND)
                def _():
                    own(kbuf, h - K_BEHIND, 4)

        @pl.when(chip == 1)
        def _():
            for h in heads:
                own(vbuf, h, 7, v_relay)
                own(kbuf, h, 6)

    def send_near(h):
        @pl.when(chip == 2)
        def _():
            own(kbuf, h, 6)
            own(vbuf, h, 7)

    def send_transit(h):
        @pl.when(chip == 1)
        def _():
            own(kbuf, h, 4)

    def project_kv(heads):
        with jax.named_scope("wkv_wait"):
            for h in heads:
                kv_wait(h)
        with jax.named_scope("kv_step"):
            both = [jnp.dot(h_v[...], wkv_v[h], preferred_element_type=F32) for h in heads]
            for h, kv in zip(heads, both):
                kbuf[h, me] = head_norm_rotate(kv[:, :hd], k_gain)
                vbuf[h, me] = kv[:, hd:].T.astype(BF16)
        for h in heads:
            own(kbuf, h, sibling)
            own(vbuf, h, sibling)
        send_wide(heads)

    project_kv([0])
    send_near(0)
    kv_start(6)
    kv_start(7)
    project_kv([1])
    send_near(1)
    wq_copy(0).start()

    def kv_pair(p, carry):
        wq_copy(p).start()
        project_kv([2 * p, 2 * p + 1])
        return carry

    lax.fori_loop(1, n_pairs, kv_pair, 0)

    @pl.when(chip == 0)
    def _():
        for h in range(n_kv - K_BEHIND, n_kv):
            own(kbuf, h, 4)

    def q_dot(h):
        qraw[lax.rem(h, 2)] = jnp.dot(h_v[...], wq_v[lax.rem(h, wq_slots)], preferred_element_type=F32)

    def q_finish(h, slot):
        q = qraw[slot]
        for g in range(group):
            qbuf[h, g * rows:(g + 1) * rows, :] = head_norm_rotate(q[:, g * hd:(g + 1) * hd], q_gain)

    def wq_wait(h):
        with jax.named_scope("wq_wait"):
            wq_copy(h).wait()

    def relay(h, c):
        @pl.when((chip == c) & (core == 1))
        @jax.named_scope("relay")
        def _():
            blocks = pl.ds(2 * (c - 2), 2)
            arrived(vbuf, h, 2, v_relay)
            push(vbuf, h, blocks, sibling, fwd_send).start()
            push(vbuf, h, blocks, 11 - 2 * c, relay_send).start()
            if c == 3:
                push(vbuf, h, blocks, 4, relay_send).start()

    def direct_k(h):
        for c in range(chips):
            @pl.when((chip == c) & (core == 0))
            @jax.named_scope("direct_k")
            def _():
                arrived(kbuf, h, 2 * c + 1)
                if c:
                    push(kbuf, h, pl.ds(0, 2 * c), sibling, fwd_send).start()

    def direct_v(h, those=range(4)):
        for c in those:
            @pl.when((chip == c) & (core == 1))
            @jax.named_scope("direct_v")
            def _():
                if c < 2:
                    arrived(vbuf, h, 2 * c + 1)
                    if c:
                        push(vbuf, h, pl.ds(0, 2), sibling, fwd_send).start()
                elif c == 3:
                    arrived(vbuf, h, 5)
                    push(vbuf, h, pl.ds(0, 2), sibling, fwd_send).start()
                    push(vbuf, h, pl.ds(4, 2), sibling, fwd_send).start()

    def wait_k(h, c):
        @pl.when(core == 1)
        @jax.named_scope("wait_k")
        def _():
            arrived(kbuf, h, 2 * c + 1)

    def wait_v(h, c):
        @pl.when(core == 0)
        @jax.named_scope("wait_v")
        def _():
            arrived(vbuf, h, 2 * c + 1)

        if c == 2:
            @pl.when(core == 1)
            @jax.named_scope("wait_v")
            def _():
                arrived(vbuf, h, 3)

    def make_scores(h, c, s_out, top_out):
        n_keys = 2 * (c + 1) * rows
        keys = kbuf[h, 0:2 * (c + 1)].reshape(n_keys, hd)
        key_id = lax.broadcasted_iota(jnp.int32, (2 * rows, rows), 0)
        row_id = lax.broadcasted_iota(jnp.int32, (2 * rows, rows), 1)
        visible = jnp.concatenate([key_id <= row_id + core * rows] * group, axis=1)
        scores = lax.dot_general(keys, qbuf[h], (((1,), (1,)), ((), ())), preferred_element_type=F32)
        last = jnp.where(visible, scores[n_keys - 2 * rows:], -jnp.inf)
        scores = jnp.concatenate([scores[:n_keys - 2 * rows], last], axis=0) if c else last
        s_out[0:n_keys, :] = scores
        top_out[...] = jnp.broadcast_to(jnp.max(scores, axis=0, keepdims=True), top_out.shape)

    def mix(h, c, s_in, top_in):
        n_keys = 2 * (c + 1) * rows
        vals = jnp.concatenate([vbuf[h, src] for src in range(2 * (c + 1))], axis=1)
        probs = jnp.exp2((s_in[0:n_keys, :] - top_in[0:1, :]) * score_scale)
        total = jnp.sum(probs, axis=0, keepdims=True)
        mixed = jnp.dot(vals, probs.astype(BF16), preferred_element_type=F32)
        mixed_t[...] = (mixed / total).astype(BF16)

    def project_out(slot):
        mixed = jnp.concatenate([mixed_t[:, g * rows:(g + 1) * rows].T for g in range(group)], axis=1)
        res[...] += jnp.dot(mixed, wo_v[slot], preferred_element_type=F32)

    def relay_step(h):
        relay(h, 2)

        @pl.when(h + AHEAD < n_kv)
        def _():
            send_near(h + AHEAD)
        send_transit(h)

    def q_step(h, carry):
        wq_wait(h)

        @pl.when(h < n_kv - 4)
        def _():
            wq_copy(h + 4).start()

        @pl.when(h >= n_kv - 4)
        def _():
            wo_copy(h - (n_kv - 4)).start()

        with jax.named_scope("q_step"):
            q_finish(jnp.maximum(h - 1, 0), lax.rem(h + 1, 2))
            q_dot(h)
            some = pl.ds(pl.multiple_of(h * 16, 16), 16)
            res[some, :] = x_v[some, :].astype(F32)

        @pl.when(h == 0)
        def _():
            relay_step(0)

        @pl.when(lax.rem(h, 3) == 1)
        def _():
            relay_step(h // 3 + 1)

        @pl.when((h == n_kv - 5) | (h == n_kv - 3) | (h == n_kv - 1))
        def _():
            relay(h // 2 - 1, 3)

        @pl.when((h == n_kv - 5) | (h == n_kv - 3))
        def _():
            direct_k(h // 2 - 1)

        @pl.when(h == n_kv - 2)
        def _():
            direct_v(0)
        return carry

    lax.fori_loop(0, n_kv, q_step, 0)
    with jax.named_scope("wo_wait"):
        wo_copy(0).wait()
    mixed_t[...] = jnp.zeros_like(mixed_t)

    for c in range(chips):
        @pl.when(chip == c)
        def _():
            wait_k(0, c)
            with jax.named_scope("first_scores"):
                make_scores(0, c, s_even, top_even)
                q_finish(n_kv - 1, (n_kv - 1) % 2)

    def head_step(h, this, other, tail):
        @pl.when(h < n_kv - 2)
        def _():
            direct_k(h + 2)

        @pl.when((h > 0) & (h < n_kv - 2))
        def _():
            relay(h + 2, 3)

        @pl.when(h < n_kv - 2)
        def _():
            direct_v(h + 1, range(chips - 1))

        @pl.when(h < n_kv - 1)
        def _():
            direct_v(h + 1, [chips - 1])

        @pl.when(h > 1)
        @jax.named_scope("wo_wait")
        def _():
            wo_copy(h - 1).wait()

        for c in range(chips):
            @pl.when(chip == c)
            def _():
                def block(more):
                    wait_v(h, c)
                    if more:
                        wait_k(h + 1, c)
                    with jax.named_scope("attend"):
                        if more:
                            project_out(lax.rem(jnp.maximum(h - 1, 0), wo_slots))
                            make_scores(h + 1, c, *other)
                        mix(h, c, *this)

                if not tail:
                    block(True)
                else:
                    @pl.when(h < n_kv - 1)
                    def _():
                        block(True)

                    @pl.when(h == n_kv - 1)
                    def _():
                        if c >= chips - 2:
                            wait_v(h, c)
                            with jax.named_scope("attend"):
                                project_out((n_kv - 2) % wo_slots)
                                mix(h, c, *this)
                        else:
                            with jax.named_scope("project"):
                                project_out((n_kv - 2) % wo_slots)
                            block(False)

        if not tail:
            @pl.when(h == n_kv - 2)
            def _():
                direct_v(n_kv - 1, range(chips - 1))

        @pl.when((h > 0) & (h < n_kv - 3))
        def _():
            wo_copy(h + 3).start()

        @pl.when(h < n_kv - 4)
        def _():
            relay_step(h + 4)

    def two_heads(i, carry):
        head_step(2 * i, (s_even, top_even), (s_odd, top_odd), False)
        head_step(2 * i + 1, (s_odd, top_odd), (s_even, top_even), True)
        return carry

    lax.fori_loop(0, n_kv // 2, two_heads, 0)
    wo_copy(n_kv - 1).wait()
    with jax.named_scope("project"):
        project_out((n_kv - 1) % wo_slots)
        out_v[...] = res[...].astype(BF16)

    def sent(buf, heads, blocks, sem):
        part = buf.at[0:heads, 0:blocks]
        pltpu.make_async_remote_copy(src_ref=part, dst_ref=part, send_sem=sem, recv_sem=k_recv.at[0],
                                     device_id={"sp": sibling}, device_id_type=MESH).wait_send()

    with jax.named_scope("finish_sends"):
        for c in range(chips):
            @pl.when(chip == c)
            def _():
                sent(kbuf, n_kv, (4, 3, 2, 1)[c], own_send.at[0])
                sent(vbuf, n_kv, (3, 2, 2, 1)[c], own_send.at[1])
                if c in (1, 3):
                    sent(kbuf, n_kv, 2 * c, fwd_send)
                if c == 2:
                    @pl.when(core == 0)
                    def _():
                        sent(kbuf, n_kv, 4, fwd_send)

                    @pl.when(core == 1)
                    def _():
                        sent(vbuf, n_kv, 2, fwd_send)
                        sent(vbuf, n_kv, 2, relay_send)
                if c == 3:
                    @pl.when(core == 1)
                    def _():
                        sent(vbuf, n_kv, 4, relay_send)


def write_back(res_v, out_hbm, sem):
    copy = pltpu.make_async_copy(res_v, out_hbm, sem)
    copy.start()
    copy.wait()


def solution(mesh):
    def device_step(hidden, ln_gain, w_q, w_k, w_v, w_o, q_gain, k_gain):
        rows, d = hidden.shape
        hd = q_gain.shape[0]
        n_kv = w_k.shape[1] // hd
        group = w_q.shape[1] // w_k.shape[1]
        n_dev = mesh.shape['sp']
        table = jnp.asarray(rope_table(rows * n_dev, hd))
        any_spec = pl.BlockSpec(memory_space=pl.ANY)
        vmem_spec = pl.BlockSpec(memory_space=pltpu.VMEM)
        dma = pltpu.SemaphoreType.DMA
        result = pl.pallas_call(
            kernel,
            out_shape=pltpu.VMEM((rows, d), BF16),
            in_specs=[any_spec] * 9,
            out_specs=vmem_spec,
            scratch_shapes=[
                pltpu.VMEM((rows, d), BF16),
                pltpu.VMEM((rows, d), BF16),
                pltpu.VMEM((d // LANES, LANES), BF16),
                pltpu.VMEM((1, hd), BF16),
                pltpu.VMEM((1, hd), BF16),
                pltpu.VMEM((rows, hd), F32),
                pltpu.VMEM((n_kv, d, 2 * hd), BF16),
                pltpu.VMEM((5, d, group * hd), BF16),
                pltpu.VMEM((4, group * hd, d), BF16),
                pltpu.VMEM((n_kv, n_dev, rows, hd), BF16),
                pltpu.VMEM((n_kv, n_dev, hd, rows), BF16),
                pltpu.VMEM((2, rows, group * hd), F32),
                pltpu.VMEM((n_kv, group * rows, hd), BF16),
                pltpu.VMEM((hd, group * rows), BF16),
                pltpu.VMEM((rows, d), F32),
                pltpu.VMEM((rows * n_dev, group * rows), F32),
                pltpu.VMEM((rows * n_dev, group * rows), F32),
                pltpu.VMEM((8, group * rows), F32),
                pltpu.VMEM((8, group * rows), F32),
                dma((5,)),
                dma((KV_FLIGHT,)),
                dma((5,)),
                dma((4,)),
                dma((2,)),
                dma,
                dma,
                dma((n_kv,)),
                dma((n_kv,)),
                dma((n_kv,)),
            ],
            compiler_params=pltpu.CompilerParams(collective_id=0, has_side_effects=True, vmem_limit_bytes=62000000),
        )(hidden, ln_gain.reshape(-1, LANES), w_q, w_k, w_v, w_o, q_gain.reshape(1, -1), k_gain.reshape(1, -1), table)
        return pl.pallas_call(
            write_back,
            out_shape=jax.ShapeDtypeStruct((rows, d), BF16),
            in_specs=[vmem_spec],
            out_specs=any_spec,
            scratch_shapes=[dma],
            compiler_params=pltpu.CompilerParams(vmem_limit_bytes=1000000),
        )(result)

    row_spec = P(('dp', 'sp'), None)
    return jax.shard_map(device_step, mesh=mesh, in_specs=(row_spec, P(), P(), P(), P(), P(), P(), P()), out_specs=row_spec, check_vma=False)
```
